32 devices in a mesh: gx: 4 (over y, x), gy: 4 (over z), gz: 2 (over core).
Axes of the slice: x: 2, y: 2, z: 4, core: 2. Of those that a mesh axis runs over, the one named last changes fastest.
Arguments:
- load: float32 [256, 256, 256], P('gx', 'gy', 'gz'), may hold values from -12 to 12
- stiffness: float32 [256, 256, 256], P('gx', 'gy', 'gz'), may hold values from 0.02 to 2
- prestress: float32 [256, 256], P(('gx', 'gy'), 'gz'), may hold values from -3 to 3
- state_var: float32 [256, 256], P(('gx', 'gy'), 'gz'), may hold values from -1 to 1
- normal_a: float32 [256, 256], P(('gx', 'gy'), 'gz'), may hold values from 1 to 3
Outputs:
- displacement: float32 [256, 256, 256], P('gx', 'gy', 'gz')
- slip_rate: float32 [256, 256], P(('gx', 'gy'), 'gz')
The draws below stay inside these ranges and needn't reach their ends.
All inputs are finite; a program needn't handle non-finite values.
Results may differ from the reference program's by a relative error of at most 0.0003.
Values sent between devices are 32-bit elements; how exact they have to be, the bound alone decides.
A program may use at most 128 MiB of HBM per device.

```python
import math
import jax
import jax.numpy as jnp

ITERS = 3
NX = 256
NY = 256
NZ = 256


def draw_load(key, part):
    subkeys = jax.random.split(key, 4)
    along_x = ((jnp.arange(NX, dtype=jnp.float32) + 0.5) / NX)[:, None, None]
    along_y = ((jnp.arange(NY, dtype=jnp.float32) + 0.5) / NY)[None, :, None]
    along_z = ((jnp.arange(NZ, dtype=jnp.float32) + 0.5) / NZ)[None, None, :]
    waves_x = jax.random.randint(subkeys[0], (4,), 1, 4).astype(jnp.float32)
    waves_z = jax.random.randint(subkeys[1], (4,), 0, 2).astype(jnp.float32)
    phases = jax.random.uniform(subkeys[2], (7,), jnp.float32, 0.0, 2.0 * math.pi)
    smooth = jnp.zeros((NX, NY, NZ), jnp.float32)
    for mode_num in range(4):
        smooth = smooth + jnp.cos(2.0 * math.pi * (waves_x[mode_num] * along_x + along_y + waves_z[mode_num] * along_z) + phases[mode_num])
    smooth = smooth * 0.7071
    exponent = 0.5 + 0.25 * jnp.sin(2.0 * math.pi * along_x + phases[4]) + 0.25 * jnp.sin(2.0 * math.pi * along_y + phases[5])
    rough_scale = 0.3 * jnp.exp(exponent * math.log(5.0))
    smooth_scale = 0.4 + 0.4 * (1.0 + jnp.cos(2.0 * math.pi * along_z + phases[6]))
    white_noise = jax.random.truncated_normal(subkeys[3], -4.0, 4.0, (NX, NY, NZ), jnp.float32)
    return (smooth_scale * smooth + rough_scale * white_noise).astype(jnp.float32)


def level_of(rng, shape, cuts, smallest, top_value):
    factor_of = 1.0
    for dim, blocks in cuts:
        steps = jax.random.uniform(jax.random.fold_in(jax.random.fold_in(rng, 6), dim), (blocks,), jnp.float32, smallest / len(cuts), top_value / len(cuts))
        factor_of = factor_of * jnp.repeat(jnp.exp(steps), shape[dim] // blocks).reshape((-1,) + (1,) * (len(shape) - 1 - dim))
    return factor_of


def bell_draw(key, shape, spread, limit, cuts=(), kind=jnp.bfloat16):
    result = spread * jax.random.normal(key, shape, jnp.float32)
    if cuts:
        result = result * level_of(key, shape, cuts, -0.22, 0.18)
    return jnp.clip(result, -limit, limit).astype(kind)


def setup_inputs(seed: int = 0) -> dict:
    key_list = jax.random.split(jax.random.key(seed), 6)
    return {
        "load": draw_load(jax.random.fold_in(key_list[5], 71), 0),
        "stiffness": jnp.clip(jnp.exp(math.log(2.0) - 4.6051702 * jax.random.uniform(key_list[1], (NX, NY, NZ), jnp.float32) ** level_of(key_list[1], (NX, NY, NZ), ((0, 4), (1, 4), (2, 2)), -0.2, 0.2)), 0.02, 2.0),
        "prestress": bell_draw(key_list[2], (NX, NZ), 1.0, 3.0, ((0, 16), (1, 2)), jnp.float32),
        "state_var": jnp.clip(jax.random.uniform(key_list[3], (NX, NZ), jnp.float32, -1.0, 1.0) * level_of(key_list[3], (NX, NZ), ((0, 16), (1, 2)), -0.4, 0.0), -1.0, 1.0),
        "normal_a": jnp.clip(jnp.exp(math.log(3.0) - 1.0986123 * jax.random.uniform(key_list[4], (NX, NZ), jnp.float32) ** level_of(key_list[4], (NX, NZ), ((0, 16), (1, 2)), -0.2, 0.2)), 1.0, 3.0),
    }


def shifted(padded, sizes_now, axis_num, offset):
    slicers = [slice(2, 2 + sizes_now[0]), slice(2, 2 + sizes_now[1]), slice(2, 2 + sizes_now[2])]
    slicers[axis_num] = slice(2 + offset, 2 + offset + sizes_now[axis_num])
    return padded[tuple(slicers)]


def operate(field, stiffness):
    padded = jnp.pad(field, 2)
    sizes_now = field.shape
    near_sum = jnp.zeros_like(field)
    for axis_num in range(3):
        near_sum = near_sum + 16.0 * (shifted(padded, sizes_now, axis_num, 1) + shifted(padded, sizes_now, axis_num, -1))
        near_sum = near_sum - (shifted(padded, sizes_now, axis_num, 2) + shifted(padded, sizes_now, axis_num, -2))
    return (7.5 + stiffness) * field - near_sum / 12.0


def reference(load, stiffness, prestress, state_var, normal_a):
    inverse = 1.0 / (7.5 + stiffness)
    solution = jnp.zeros_like(load)
    residual = load
    precond = inverse * residual
    direction = precond
    gamma = jnp.sum(residual * precond)
    for iteration in range(ITERS):
        image = operate(direction, stiffness)
        alpha = gamma / jnp.sum(direction * image)
        solution = solution + alpha * direction
        residual = residual - alpha * image
        if iteration + 1 < ITERS:
            precond = inverse * residual
            gamma_new = jnp.sum(residual * precond)
            direction = precond + (gamma_new / gamma) * direction
            gamma = gamma_new
    half = NY // 2
    traction = (solution[:, half - 2, :] - 27.0 * solution[:, half - 1, :]
                + 27.0 * solution[:, half, :] - solution[:, half + 1, :]) / 24.0
    slip_rate = jnp.exp(-state_var) * jnp.sinh((prestress + 2.0 * traction) / normal_a)
    return solution, slip_rate
```

```python
import jax
import jax.numpy as jnp
from jax import lax
from jax.experimental import pallas as pl
from jax.experimental.pallas import tpu as pltpu
from jax.sharding import PartitionSpec as P

MESH = pl.DeviceIdType.MESH
AXES = ("gx", "gy", "gz")
PAD = 8
CHUNK = 8
GROUP = 2


def total(values):
    return jnp.sum(values.reshape(-1, 8, values.shape[-1]), axis=0)


def solve(t0, s):
    t1 = t0 - s[0]
    t2 = t1 - s[1]
    tiny = 1e-7
    p0 = s[0]
    l10 = s[1] / p0
    l20 = s[2] / p0
    p1 = s[2] - l10 * s[1]
    q = s[3] - l20 * s[1]
    ok1 = p1 > tiny * s[2]
    i1 = jnp.where(ok1, 1.0 / jnp.where(ok1, p1, 1.0), 0.0)
    l21 = q * i1
    p2 = s[4] - l20 * s[2] - l21 * q
    ok2 = ok1 & (p2 > tiny * s[4])
    i2 = jnp.where(ok2, 1.0 / jnp.where(ok2, p2, 1.0), 0.0)
    y1 = t1 - l10 * t0
    y2 = t2 - l20 * t0 - l21 * y1
    c2 = y2 * i2
    c1 = y1 * i1 - l21 * c2
    c0 = t0 / p0 - l10 * c1 - l20 * c2
    return c0, c1, c2


def parts_of(nx):
    inner = nx - 4
    runs = max(n for n in range(1, 7) if inner % (GROUP * n) == 0)
    size = inner // runs
    return [(0, 2), (nx - 2, 2)] + [(2 + n * size, size) for n in range(runs)]


def halves(values):
    high = values.astype(jnp.bfloat16)
    return high, (values - high.astype(jnp.float32)).astype(jnp.bfloat16)


def make_kernel(sizes):
    ngx, ngy, ngz = sizes
    count = ngx * ngy * ngz

    def kernel(load, stiff, u0, u1, u2, coef_ref, frecv,
               b, d, ysend, yrecv, zrecv, band, zterm, fsend, red,
               in_sem, send_sem, recv_sem, zs_sem, zr_sem, fs_sem, fr_sem, rs_sem, rr_sem,
               row_sem, all_sem):
        nx, ny, nz = b.shape
        us = (u0, u1, u2)
        ix, iy, iz = (lax.axis_index(a) for a in AXES)
        me = (ix * ngy + iy) * ngz + iz

        def around(spot, size):
            moved = [spot + n for n in range(size)]
            return [spot] + [jnp.where(m >= size, m - size, m) for m in moved[1:]]

        xs, ys, zs = around(ix, ngx), around(iy, ngy), around(iz, ngz)

        parts = parts_of(nx)
        copies = []
        for n, (at, size) in enumerate(parts):
            part = pl.ds(at, size)
            copies.append((
                pltpu.make_async_copy(load.at[part], b.at[part], in_sem.at[0, n]),
                pltpu.make_async_copy(stiff.at[part], d.at[part], in_sem.at[1, n]),
            ))
            for one in copies[n]:
                one.start()

        barrier = pltpu.get_barrier_semaphore()

        in_line = ([(ix, iy, z) for z in zs[1:]] + [(x, iy, iz) for x in xs[1:]]
                   + [(ix, y, iz) for y in ys[1:]])
        for who in in_line:
            pl.semaphore_signal(barrier, inc=1, device_id=who, device_id_type=MESH)

        zero_plane = jnp.zeros((2, ny, nz), jnp.float32)
        zero_rows = jnp.zeros((nx, 2, nz), jnp.float32)
        for k in range(3):
            @pl.when(ix == 0)
            def _():
                us[k][0:2, PAD:PAD + ny, :] = zero_plane
            @pl.when(ix == ngx - 1)
            def _():
                us[k][nx + 2:nx + 4, PAD:PAD + ny, :] = zero_plane
            @pl.when(iy == 0)
            def _():
                yrecv[k, 0] = zero_rows
            @pl.when(iy == ngy - 1)
            def _():
                yrecv[k, 1] = zero_rows

        row = lax.broadcasted_iota(jnp.int32, (nz, nz), 0)
        col = lax.broadcasted_iota(jnp.int32, (nz, nz), 1)
        far = row + jnp.where(iz == 0, nz, -nz)
        for n, at in enumerate((row, far, row, far)):
            gap = col - at
            full = jnp.where(jnp.abs(gap) == 1, 16.0, 0.0) - jnp.where(jnp.abs(gap) == 2, 1.0, 0.0)
            half = jnp.where(gap == 1, 16.0, 0.0) - jnp.where(gap == 2, 1.0, 0.0)
            band[0, n * nz:(n + 1) * nz, :] = full.astype(jnp.bfloat16)
            band[1, n * nz:(n + 1) * nz, :] = half.astype(jnp.bfloat16)

        def place(x, value, k):
            us[k][x + 2, PAD:PAD + ny, :] = value
            ysend[k, 0, x] = value[0:2]
            ysend[k, 1, x] = value[ny - 2:ny]

        def xcopy(k, side):
            u = us[k]
            if side == 0:
                src, dst, to = u.at[2:4, PAD:PAD + ny], u.at[nx + 2:nx + 4, PAD:PAD + ny], ix - 1
            else:
                src, dst, to = u.at[nx:nx + 2, PAD:PAD + ny], u.at[0:2, PAD:PAD + ny], ix + 1
            return pltpu.make_async_remote_copy(
                src, dst, send_sem.at[k, side], recv_sem.at[k, side],
                device_id=(to, iy, iz), device_id_type=MESH)

        def ycopy(k, side):
            to = iy - 1 if side == 0 else iy + 1
            return pltpu.make_async_remote_copy(
                ysend.at[k, side], yrecv.at[k, 1 - side], send_sem.at[k, 2 + side],
                recv_sem.at[k, 2 + side], device_id=(ix, to, iz), device_id_type=MESH)

        strips = ((8, ny - 8), (0, 8), (ny - 8, ny))

        def zcopy(k, at, size, n, strip):
            lo, hi = (0, ny) if strip is None else strips[strip]
            which = 0 if strip is None else strip
            return pltpu.make_async_remote_copy(
                us[k].at[pl.ds(at + 2, size), PAD + lo:PAD + hi], zrecv.at[k, pl.ds(at, size), lo:hi],
                zs_sem.at[k, n, which], zr_sem.at[k, n, which],
                device_id=(ix, iy, 1 - iz), device_id_type=MESH)

        def strips_of(n):
            return (None,) if n < 2 else (0, 1, 2)

        def sending(spot, size, side):
            return spot > 0 if side == 0 else spot < size - 1

        def receiving(spot, size, side):
            return spot < size - 1 if side == 0 else spot > 0

        def sides(k):
            return (1,) if k == 2 else (0, 1)

        def each(make, k, spot, size, test, act):
            for side in sides(k):
                @pl.when(test(spot, size, side))
                def _():
                    act(make(k, side))

        def start_x(k):
            each(xcopy, k, ix, ngx, sending, lambda c: c.start())

        def start_y(k):
            each(ycopy, k, iy, ngy, sending, lambda c: c.start())

        def scale(x, t0):
            inv = 1.0 / (7.5 + d[x])
            d[x] = inv
            rhs = b[x]
            value = inv * rhs
            place(x, value, 0)
            return t0 + total(value * rhs)

        t0 = jnp.zeros((8, nz), jnp.float32)
        for n, (at, size) in enumerate(parts):
            for one in copies[n]:
                one.wait()
            t0 = lax.fori_loop(at, at + size, scale, t0)
            if n == 1:
                pl.semaphore_wait(barrier, len(in_line))
                for y in ys[1:]:
                    pl.semaphore_signal(row_sem, inc=1, device_id=(ix, y, iz), device_id_type=MESH)
                start_x(0)
                zcopy(0, *parts[0], 0, None).start()
            if n >= 1:
                for strip in strips_of(n):
                    zcopy(0, at, size, n, strip).start()
        start_y(0)

        def wait_y(k):
            each(ycopy, k, iy, ngy, receiving, lambda c: c.wait_recv())

        def wait_x(k):
            each(xcopy, k, ix, ngx, receiving, lambda c: c.wait_recv())

        def along_z(k, at, size, lo, hi, which):
            rows = size * (hi - lo)
            own = us[k][pl.ds(at + 2, size), PAD + lo:PAD + hi, :].reshape(rows, nz)
            next_to = zrecv[k, pl.ds(at, size), lo:hi, :].reshape(rows, nz)
            own_high, own_low = halves(own)
            next_high, next_low = halves(next_to)
            lhs = jnp.concatenate([own_high, next_high, own_low, next_low], axis=1)
            found = jnp.dot(lhs, band[which], preferred_element_type=jnp.float32)
            zterm[pl.ds(at, size), lo:hi, :] = found.reshape(size, hi - lo, nz)

        def near(k, x, lo, hi):
            u = us[k]
            lo, hi = lo + PAD, hi + PAD
            one = (u[x + 1, lo:hi, :] + u[x + 3, lo:hi, :]
                   + u[x + 2, lo - 1:hi - 1, :] + u[x + 2, lo + 1:hi + 1, :])
            two = (u[x, lo:hi, :] + u[x + 4, lo:hi, :]
                   + u[x + 2, lo - 2:hi - 2, :] + u[x + 2, lo + 2:hi + 2, :])
            return (16.0 * one - two + zterm[x, lo - PAD:hi - PAD, :]) * (1.0 / 12.0)

        def half_near(k, x, lo, hi):
            u = us[k]
            lo, hi = lo + PAD, hi + PAD
            one = u[x + 1, lo:hi, :] + u[x + 2, lo - 1:hi - 1, :]
            two = u[x, lo:hi, :] + u[x + 2, lo - 2:hi - 2, :]
            return (16.0 * one - two + zterm[x, lo - PAD:hi - PAD, :]) * (1.0 / 6.0)

        zero = jnp.zeros((8, nz), jnp.float32)

        def run(block, k, carry, which, finish):
            first_at, size = parts[2]

            def part(n, carry):
                at = first_at + n * size
                zcopy(k, at, size, n + 2, 0).wait_recv()
                along_z(k, at, size, *strips[0], which)

                def inner(i, carry):
                    for g in range(GROUP):
                        carry = block(at + i * GROUP + g, *strips[0], carry)
                    return carry

                carry = lax.fori_loop(0, size // GROUP, inner, carry)
                if k < 2:
                    zcopy(k + 1, at, size, n + 2, 0).start()
                return carry

            carry = lax.fori_loop(0, len(parts) - 2, part, carry)
            for n, (at, size) in enumerate(parts):
                for strip in strips_of(n):
                    if strip != 0:
                        zcopy(k, at, size, n, strip).wait_recv()
                if n < 2:
                    along_z(k, at, size, 0, ny, which)
            for strip in (1, 2):
                along_z(k, 2, nx - 4, *strips[strip], which)
            wait_y(k)

            def rim(i, carry):
                for g in range(GROUP):
                    x = i * GROUP + g
                    us[k][x + 2, PAD - 2:PAD, :] = yrecv[k, 0, x]
                    us[k][x + 2, PAD + ny:PAD + ny + 2, :] = yrecv[k, 1, x]
                    carry = block(x, 0, 8, carry)
                    carry = block(x, ny - 8, ny, carry)
                return carry

            def whole(n, carry):
                x = jnp.where(n < 2, n, nx - 4 + n)
                us[k][x + 2, PAD - 2:PAD, :] = yrecv[k, 0, x]
                us[k][x + 2, PAD + ny:PAD + ny + 2, :] = yrecv[k, 1, x]
                carry = block(x, 0, ny, carry)
                return carry

            carry = lax.fori_loop(1, nx // GROUP - 1, rim, carry)
            wait_x(k)
            carry = lax.fori_loop(0, 4, whole, carry)
            finish()
            return carry

        def advance(k):
            def block(x, lo, hi, carry):
                even, odd = carry
                value = us[k][x + 2, PAD + lo:PAD + hi, :]
                w = near(k, x, lo, hi)
                fresh = d[x, lo:hi, :] * w
                even = even + total(value * (b[x, lo:hi, :] - w))
                odd = odd + total((value - fresh) * w)
                b[x, lo:hi, :] = w
                us[k + 1][x + 2, PAD + lo:PAD + hi, :] = fresh
                if lo == 0:
                    ysend[k + 1, 0, x] = fresh[0:2]
                if hi == ny:
                    ysend[k + 1, 1, x] = fresh[hi - lo - 2:hi - lo]
                return even, odd

            def finish():
                start_x(k + 1)
                start_y(k + 1)
                for n, (at, size) in enumerate(parts):
                    for strip in strips_of(n):
                        if strip != 0:
                            zcopy(k + 1, at, size, n, strip).start()

            return run(block, k, (zero, zero), 0, finish)

        s0, s1 = advance(0)
        pl.semaphore_wait(row_sem, ngy - 1)
        for z in zs[1:]:
            pl.semaphore_signal(all_sem, inc=1, device_id=(ix, iy, z), device_id_type=MESH)
        s2, s3 = advance(1)

        owned = nx // ngy
        below = iy == ngy // 2 - 1
        above = iy == ngy // 2

        def fault_copy(which, to):
            return pltpu.make_async_remote_copy(
                fsend.at[:, pl.ds(to * owned, owned), :], frecv.at[which], fs_sem.at[to], fr_sem.at[which],
                device_id=(ix, to, iz), device_id_type=MESH)

        @pl.when(below | above)
        def _():
            edge = jnp.where(below, 1, 0)
            front = jnp.where(below, 1.0 / 24.0, 27.0 / 24.0)
            close = jnp.where(below, -27.0 / 24.0, -1.0 / 24.0)

            @pl.loop(0, nx)
            def _(x):
                for j in range(3):
                    rows = ysend[j, edge, x]
                    fsend[j, pl.ds(x, 1), :] = front * rows[0:1] + close * rows[1:2]

        for which, owner in enumerate((ngy // 2 - 1, ngy // 2)):
            @pl.when(iy == owner)
            def _():
                for to in range(ngy):
                    if to != owner:
                        fault_copy(which, to).start()
                frecv[which] = fsend[:, owner * owned:(owner + 1) * owned, :]

        def last(x, lo, hi, s4):
            value = us[2][x + 2, PAD + lo:PAD + hi, :]
            return s4 + total(value * (b[x, lo:hi, :] - half_near(2, x, lo, hi)))

        slot = lax.broadcasted_iota(jnp.int32, (1, nz), 1)

        def spread(parts):
            sent = jnp.zeros((1, nz), jnp.float32)
            for j, part in parts:
                whole = jnp.sum(jnp.sum(part, axis=0, keepdims=True), axis=1, keepdims=True)
                sent = sent + jnp.where(slot == j, whole, 0.0)
            return sent

        early = spread(list(enumerate((t0, s0, s1, s2, s3))))
        s4 = run(last, 2, zero, 1, lambda: None)
        red[me] = early + spread([(5, s4)])
        pl.semaphore_wait(all_sem, ngz - 1)

        def sum_copy(who):
            return pltpu.make_async_remote_copy(
                red.at[me], red.at[me], rs_sem, rr_sem, device_id=who, device_id_type=MESH)

        others = [(x, y, z) for y in reversed(ys) for x in reversed(xs) for z in reversed(zs)][:-1]
        for who in others:
            sum_copy(who).start()

        for which, owner in enumerate((ngy // 2 - 1, ngy // 2)):
            @pl.when(iy != owner)
            def _():
                fault_copy(which, owner).wait_recv()
        for k in range(3):
            each(xcopy, k, ix, ngx, sending, lambda c: c.wait_send())
            each(ycopy, k, iy, ngy, sending, lambda c: c.wait_send())
            for n, (at, size) in enumerate(parts):
                for strip in strips_of(n):
                    zcopy(k, at, size, n, strip).wait_send()
        for which, owner in enumerate((ngy // 2 - 1, ngy // 2)):
            @pl.when(iy == owner)
            def _():
                for to in range(ngy):
                    if to != owner:
                        fault_copy(which, to).wait_send()

        arrived = red.at[pl.ds(0, count - 1)]
        everyone = pltpu.make_async_remote_copy(
            arrived, arrived, rs_sem, rr_sem, device_id=others[0], device_id_type=MESH)
        everyone.wait_recv()
        sums = jnp.sum(red[...], axis=0)
        sums = [jnp.sum(jnp.where(slot == j, sums, 0.0), axis=1, keepdims=True) for j in range(6)]
        coefs = solve(sums[0], sums[1:])
        for j in range(3):
            coef_ref[j:j + 1, :] = jnp.broadcast_to(coefs[j], (1, nz))
        everyone.wait_send()

    return kernel


def blend(u0, u1, u2, coef_ref, fault, pre_ref, state_ref, norm_ref, out, slip, obuf, out_sem):
    nx, ny, nz = obuf.shape
    mid = slice(PAD, PAD + ny)
    coefs = [coef_ref[j:j + 1, :] for j in range(3)]

    def out_copy(c):
        part = pl.ds(c * CHUNK, CHUNK)
        return pltpu.make_async_copy(obuf.at[part], out.at[part], out_sem.at[c])

    def plane(x, carry):
        obuf[x] = (coefs[0] * u0[x + 2, mid, :] + coefs[1] * u1[x + 2, mid, :]
                   + coefs[2] * u2[x + 2, mid, :])
        return carry

    for c in range(nx // CHUNK):
        lax.fori_loop(c * CHUNK, (c + 1) * CHUNK, plane, 0)
        out_copy(c).start()
    traction = sum(coefs[j] * (fault[0, j] + fault[1, j]) for j in range(3))
    arg = (pre_ref[...] + 2.0 * traction) / norm_ref[...]
    half = jnp.float32(-0.6931471805599453)
    small = arg * (1.0 + arg * arg * (1.0 / 6.0) * (1.0 + arg * arg * 0.05))
    sinh = jnp.where(jnp.abs(arg) < 0.25, small, jnp.exp(arg + half) - jnp.exp(half - arg))
    slip[...] = jnp.exp(-state_ref[...]) * sinh
    for c in range(nx // CHUNK):
        out_copy(c).wait()


def solution(mesh):
    sizes = tuple(mesh.shape[a] for a in AXES)
    assert sizes[1] % 2 == 0 and sizes[2] == 2

    def per_device(load, stiffness, prestress, state_var, normal_a):
        nx, ny, nz = load.shape
        assert nx % CHUNK == 0
        runs = len(parts_of(nx))
        f32 = jnp.float32
        count = sizes[0] * sizes[1] * sizes[2]
        padded = (nx + 4, ny + 2 * PAD, nz)
        vmem = pl.BlockSpec(memory_space=pltpu.VMEM)
        hbm = pl.BlockSpec(memory_space=pltpu.HBM)
        dma = pltpu.SemaphoreType.DMA
        u0, u1, u2, coefs, fault = pl.pallas_call(
            make_kernel(sizes),
            out_shape=(
                pltpu.VMEM(padded, f32),
                pltpu.VMEM(padded, f32),
                pltpu.VMEM(padded, f32),
                pltpu.VMEM((8, nz), f32),
                pltpu.VMEM((2, 3, nx // sizes[1], nz), f32),
            ),
            in_specs=[hbm, hbm],
            out_specs=(vmem,) * 5,
            scratch_shapes=[
                pltpu.VMEM((nx, ny, nz), f32),
                pltpu.VMEM((nx, ny, nz), f32),
                pltpu.VMEM((3, 2, nx, 2, nz), f32),
                pltpu.VMEM((3, 2, nx, 2, nz), f32),
                pltpu.VMEM((3, nx, ny, nz), f32),
                pltpu.VMEM((2, 4 * nz, nz), jnp.bfloat16),
                pltpu.VMEM((nx, ny, nz), f32),
                pltpu.VMEM((3, nx, nz), f32),
                pltpu.VMEM((count, 1, nz), f32),
                dma((2, runs)),
                dma((3, 4)),
                dma((3, 4)),
                dma((3, runs, 3)),
                dma((3, runs, 3)),
                dma((sizes[1],)),
                dma((2,)),
                dma,
                dma,
                pltpu.SemaphoreType.REGULAR,
                pltpu.SemaphoreType.REGULAR,
            ],
            compiler_params=pltpu.CompilerParams(
                collective_id=0, has_side_effects=True, vmem_limit_bytes=54 * 2**20),
        )(load, stiffness)
        displacement, slip = pl.pallas_call(
            blend,
            out_shape=(
                jax.ShapeDtypeStruct(load.shape, f32),
                jax.ShapeDtypeStruct(prestress.shape, f32),
            ),
            in_specs=[vmem] * 8,
            out_specs=(hbm, vmem),
            scratch_shapes=[pltpu.VMEM((nx, ny, nz), f32), dma((nx // CHUNK,))],
            compiler_params=pltpu.CompilerParams(vmem_limit_bytes=8 * 2**20),
        )(u0, u1, u2, coefs, fault, prestress, state_var, normal_a)
        return displacement, slip

    placed = (
        P("gx", "gy", "gz"),
        P("gx", "gy", "gz"),
        P(("gx", "gy"), "gz"),
        P(("gx", "gy"), "gz"),
        P(("gx", "gy"), "gz"),
    )
    return jax.shard_map(
        per_device,
        mesh=mesh,
        in_specs=placed,
        out_specs=(P("gx", "gy", "gz"), P(("gx", "gy"), "gz")),
        check_vma=False,
    )
```

```python
import functools
import itertools
import jax
import jax.numpy as jnp
from jax import lax
from jax.experimental import pallas as pl
from jax.experimental.pallas import tpu as pltpu
from jax.sharding import PartitionSpec as P

MESH = pl.DeviceIdType.MESH
AXES = ("gx", "gy", "gz")
PAD = 8
CHUNK = 8
LOADS = 2


def total(values):
    return jnp.sum(values.reshape(-1, 8, values.shape[-1]), axis=0)


def solve(t0, s):
    t1 = t0 - s[0]
    t2 = t1 - s[1]
    tiny = 1e-7
    p0 = s[0]
    l10 = s[1] / p0
    l20 = s[2] / p0
    p1 = s[2] - l10 * s[1]
    q = s[3] - l20 * s[1]
    ok1 = p1 > tiny * s[2]
    i1 = jnp.where(ok1, 1.0 / jnp.where(ok1, p1, 1.0), 0.0)
    l21 = q * i1
    p2 = s[4] - l20 * s[2] - l21 * q
    ok2 = ok1 & (p2 > tiny * s[4])
    i2 = jnp.where(ok2, 1.0 / jnp.where(ok2, p2, 1.0), 0.0)
    y1 = t1 - l10 * t0
    y2 = t2 - l20 * t0 - l21 * y1
    c2 = y2 * i2
    c1 = y1 * i1 - l21 * c2
    c0 = t0 / p0 - l10 * c1 - l20 * c2
    return c0, c1, c2


def divisor(n, most):
    return max(m for m in range(1, most + 1) if n % m == 0)


def halves(values):
    high = values.astype(jnp.bfloat16)
    return high, (values - high.astype(jnp.float32)).astype(jnp.bfloat16)


def radii(sizes):
    needed = sum(n - 1 for n in sizes)
    hops, reached = [], 1
    while reached < needed or len(hops) < 2:
        hops.append(min(reached, max(needed - reached, 1)))
        reached += hops[-1]
    return hops


def make_kernel(sizes):
    ngx, ngy, ngz = sizes
    count = ngx * ngy * ngz

    def kernel(load, stiff, u0, u1, u2, coef_ref, frecv,
               b, d, ysend, yrecv, zsend, zrecv, rsend, rrecv, band, zterm, fsend, red,
               in_sem, send_sem, recv_sem, zs_sem, zr_sem, fs_sem, fr_sem, rs_sem, rr_sem,
               known):
        nx, ny, nz = b.shape
        us = (u0, u1, u2)
        ix, iy, iz = (lax.axis_index(a) for a in AXES)
        me = (ix * ngy + iy) * ngz + iz
        half = (nx - 4) // 2
        size = divisor(half, 10)
        window = divisor(size, 5)
        piece = half // LOADS
        strip = divisor(nx - 4, 6)
        border_run = divisor(nx - 4, 30)
        mid = tuple(range(8, ny - 8, 8))
        ends = (0, ny - 8)
        full = tuple(range(0, ny, 8))

        def around(spot, size):
            moved = [spot + n for n in range(size)]
            return [spot] + [jnp.where(m >= size, m - size, m) for m in moved[1:]]

        xs, ys, zs = around(ix, ngx), around(iy, ngy), around(iz, ngz)

        sources = ((load, b), (stiff, d))
        for src, dst in sources:
            for at in (0, nx - 2):
                pltpu.make_async_copy(src.at[at:at + 2], dst.at[at:at + 2], in_sem.at[0]).start()
        for src, dst in sources:
            for at in ends:
                pltpu.make_async_copy(
                    src.at[2:nx - 2, at:at + 8], dst.at[2:nx - 2, at:at + 8], in_sem.at[1]).start()
        for n in range(2 * LOADS):
            part = pl.ds(2 + n * piece, piece)
            for src, dst in sources:
                pltpu.make_async_copy(
                    src.at[part, 8:ny - 8], dst.at[part, 8:ny - 8], in_sem.at[2 + n]).start()

        def loaded(ref, n):
            pltpu.make_async_copy(ref, ref, in_sem.at[n]).wait()

        barrier = pltpu.get_barrier_semaphore()
        spots = (ix, iy, iz)

        def ball(radius):
            reach = [range(-min(radius, n - 1), min(radius, n - 1) + 1) for n in sizes]
            for step in itertools.product(*reach):
                if 0 < sum(abs(g) for g in step) <= radius:
                    inside = [spot + g >= 0 if g < 0 else spot + g < n
                              for spot, g, n in zip(spots, step, sizes) if g]
                    yield functools.reduce(jnp.logical_and, inside), tuple(
                        spot + g for spot, g in zip(spots, step))

        def tell(sem, radius):
            for there, who in ball(radius):
                @pl.when(there)
                def _():
                    pl.semaphore_signal(sem, inc=1, device_id=who, device_id_type=MESH)

        def hear(sem, radius):
            pl.semaphore_wait(sem, sum(jnp.where(there, 1, 0) for there, _ in ball(radius)))

        hops = radii(sizes)
        tell(barrier, 1)

        zero_plane = jnp.zeros((2, ny, nz), jnp.float32)
        zero_rows = jnp.zeros((nx, 2, nz), jnp.float32)
        for k in range(3):
            @pl.when(ix == 0)
            def _():
                us[k][0:2, PAD:PAD + ny, :] = zero_plane
            @pl.when(ix == ngx - 1)
            def _():
                us[k][nx + 2:nx + 4, PAD:PAD + ny, :] = zero_plane
            @pl.when(iy == 0)
            def _():
                yrecv[k, 0] = zero_rows
            @pl.when(iy == ngy - 1)
            def _():
                yrecv[k, 1] = zero_rows

        row = lax.broadcasted_iota(jnp.int32, (nz, nz), 0)
        col = lax.broadcasted_iota(jnp.int32, (nz, nz), 1)
        far = jnp.bitwise_and(col, 1) + jnp.where(iz == 0, nz, -2)

        def weights(gap, near):
            return jnp.where(near(gap) == 1, 16.0, 0.0) - jnp.where(near(gap) == 2, 1.0, 0.0)

        own = weights(col - row, jnp.abs)
        up = weights(col - row, lambda g: g)
        out = weights(far - row, jnp.abs).astype(jnp.bfloat16)
        for which, part in enumerate((own, up)):
            for n in range(2):
                band[which, n * nz:(n + 1) * nz, 0:nz] = part.astype(jnp.bfloat16)
                band[which, n * nz:(n + 1) * nz, nz:2 * nz] = out

        lane = lax.broadcasted_iota(jnp.int32, (8, nz), 1)
        pair = lane // 2
        edge_low = jnp.where(iz == 0, nz - 2, 0)
        at_edge = (lane >= edge_low) & (lane < edge_low + 2)
        at_upper = at_edge & (iz == 1)

        def xcopy(k, side):
            u = us[k]
            if side == 0:
                src, dst, to = u.at[2:4, PAD:PAD + ny], u.at[nx + 2:nx + 4, PAD:PAD + ny], ix - 1
            else:
                src, dst, to = u.at[nx:nx + 2, PAD:PAD + ny], u.at[0:2, PAD:PAD + ny], ix + 1
            return pltpu.make_async_remote_copy(
                src, dst, send_sem.at[k % 2, side], recv_sem.at[k % 2, side],
                device_id=(to, iy, iz), device_id_type=MESH)

        def ycopy(k, side, first=0, many=nx - 4, sem=2):
            to = iy - 1 if side == 0 else iy + 1
            part = pl.ds(first, many)
            return pltpu.make_async_remote_copy(
                ysend.at[k, side, part], yrecv.at[k, 1 - side, part], send_sem.at[k % 2, sem + side],
                recv_sem.at[k % 2, sem + side], device_id=(ix, to, iz), device_id_type=MESH)

        def corner(k, side):
            return ycopy(k, side, nx - 4, 4, 4)

        def place(x, rim):
            if not rim:
                return x - 2
            return x if x >= nx - 2 else nx - 4 + x

        def zcopy(k, n):
            src, dst = (rsend.at[k], rrecv.at[k]) if n == 2 else (zsend.at[k, n], zrecv.at[k, n])
            return pltpu.make_async_remote_copy(
                src, dst, zs_sem.at[k % 2, n], zr_sem.at[k % 2, n],
                device_id=(ix, iy, 1 - iz), device_id_type=MESH)

        def sending(spot, size, side):
            return spot > 0 if side == 0 else spot < size - 1

        def receiving(spot, size, side):
            return spot < size - 1 if side == 0 else spot > 0

        def sides(k):
            return (1,) if k == 2 else (0, 1)

        def each(make, k, spot, size, test, act):
            for side in sides(k):
                @pl.when(test(spot, size, side))
                def _():
                    act(make(k, side))

        def start_x(k):
            odd = lax.rem(ix, 2) == 1
            for side, turn in ((1, odd), (0, None), (1, jnp.logical_not(odd))):
                if side in sides(k):
                    go = sending(ix, ngx, side)
                    @pl.when(go if turn is None else go & turn)
                    def _():
                        xcopy(k, side).start()

        def start_y(k):
            each(ycopy, k, iy, ngy, sending, lambda c: c.start())

        def start_corner(k):
            each(corner, k, iy, ngy, sending, lambda c: c.start())

        def sent(k):
            each(xcopy, k, ix, ngx, sending, lambda c: c.wait_send())
            each(ycopy, k, iy, ngy, sending, lambda c: c.wait_send())
            each(corner, k, iy, ngy, sending, lambda c: c.wait_send())
            for n in range(3):
                zcopy(k, n).wait_send()

        def wait_y(k):
            each(ycopy, k, iy, ngy, receiving, lambda c: c.wait_recv())

        def wait_x(k):
            each(corner, k, iy, ngy, receiving, lambda c: c.wait_recv())
            each(xcopy, k, ix, ngx, receiving, lambda c: c.wait_recv())

        def along_z(k, values, rows):
            high, low = halves(values)
            lhs = jnp.concatenate([high, low], axis=1)
            found = jnp.dot(lhs, band[1 if k == 2 else 0], preferred_element_type=jnp.float32)
            return found[:, :nz].reshape(-1, rows, nz), found[:, nz:].reshape(-1, rows, nz)

        def picked(k, x, n, lo, hi, packed):
            rows = hi - lo
            values = us[k][pl.ds(x + 2, n), PAD + lo:PAD + hi, :].reshape(n * rows, nz)
            own, out = along_z(k, values, rows)
            zterm[pl.ds(x, n), lo:hi, :] = own
            for g in range(n):
                keep = jnp.concatenate([pair] * (rows // 8), axis=0) == x + g
                packed = jnp.where(keep, out[g], packed)
            return packed

        def rims_z(k):
            low = high = jnp.zeros((8, nz), jnp.float32)
            for h in range(2):
                low = picked(k, 2 + h * half, half, 0, 8, low)
                high = picked(k, 2 + h * half, half, ny - 8, ny, high)
            rsend[k, 0:8] = low
            rsend[k, 8:16] = high
            packed = jnp.zeros((ny, nz), jnp.float32)
            for at in (0, nx - 2):
                packed = picked(k, at, 2, 0, ny, packed)
            rsend[k, 16:16 + ny] = packed
            zcopy(k, 2).start()

        def put(k, x, slot, t, value):
            us[k][x + 2, PAD + t:PAD + t + 8, :] = value
            if t == 0:
                ysend[k, 0, slot] = value[0:2]
            if t == ny - 8:
                ysend[k, 1, slot] = value[6:8]

        def scale(x, n, tiles, t0, slot=None):
            for g in range(n):
                for t in tiles:
                    rows = slice(t, t + 8)
                    inv = 1.0 / (7.5 + d[x + g, rows])
                    rhs = b[x + g, rows]
                    value = inv * rhs
                    d[x + g, rows] = inv * (1.0 / 12.0)
                    b[x + g, rows] = 12.0 * rhs
                    put(0, x + g, x + g - 2 if slot is None else slot, t, value)
                    t0 = t0 + value * rhs
            return t0

        def shift_of(x):
            return jnp.bitwise_and(jnp.where(iz == 0, nz - 2, nz) - 2 * x, nz - 1)

        def stencil(k, x, n, tiles, source, carry, rim=False):
            u = us[k]
            for t in tiles:
                lo, hi = PAD + t, PAD + t + 8
                packed = source(t)
                line = [u[x + j, lo:hi, :] for j in range(n + 4 if k < 2 else n + 2)]
                for g in range(n):
                    at = x + g
                    rows = slice(t, t + 8)
                    c = line[g + 2]
                    z = zterm[at, rows] + jnp.where(
                        at_edge if k < 2 else at_upper, pltpu.roll(packed, shift_of(at), 1), 0.0)
                    if k < 2:
                        even, odd = carry
                        one = ((line[g + 1] + line[g + 3])
                               + (u[at + 2, lo - 1:hi - 1, :] + u[at + 2, lo + 1:hi + 1, :]))
                        two = ((line[g] + line[g + 4])
                               + (u[at + 2, lo - 2:hi - 2, :] + u[at + 2, lo + 2:hi + 2, :]))
                        w = (16.0 * one - two) + z
                        fresh = d[at, rows] * w
                        even = even + c * (b[at, rows] - w)
                        odd = odd + (c - fresh) * w
                        b[at, rows] = w
                        put(k + 1, at, place(at, rim), t, fresh)
                        carry = even, odd
                    else:
                        one = line[g + 1] + u[at + 2, lo - 1:hi - 1, :]
                        two = line[g] + u[at + 2, lo - 2:hi - 2, :]
                        w = (16.0 * one - two) + z
                        carry = carry + c * (b[at, rows] - (w + w))
            return carry

        def inside(k, make, carry):
            for h in range(2):
                zcopy(k, h).wait_recv()

                def chunk(i, state):
                    carry, packed = state
                    x = 2 + h * half + i * size
                    carry = make(h, x, carry)
                    if k < 2:
                        packed = picked(k + 1, x, size, 8, ny - 8, packed)
                    return carry, packed

                start = jnp.zeros((ny - 16, nz), jnp.float32)
                carry, packed = lax.fori_loop(0, half // size, chunk, (carry, start))
                if k < 2:
                    zsend[k + 1, h] = packed
                    zcopy(k + 1, h).start()
            return carry

        zero = jnp.zeros((8, nz), jnp.float32)

        loaded(b.at[0:8], 0)
        t0 = lax.fori_loop(0, 4, lambda n, c: scale(
            jnp.where(n < 2, n, nx - 4 + n), 1, full, c, nx - 4 + n), zero)
        hear(barrier, 1)
        start_x(0)
        start_corner(0)
        tell(known.at[0], hops[0])
        loaded(b.at[2:nx - 2, 0:32], 1)
        t0 = lax.fori_loop(0, (nx - 4) // strip, lambda n, c: scale(2 + n * strip, strip, ends, c), t0)
        start_y(0)
        rims_z(0)

        for h in range(2):
            packed = jnp.zeros((ny - 16, nz), jnp.float32)
            for n in range(LOADS):
                first = (h * LOADS + n) * piece
                loaded(b.at[0:2 * piece, 8:ny - 8], 2 + h * LOADS + n)
                run = divisor(piece, 15)

                def chunk(i, state):
                    t0, packed = state
                    x = 2 + first + i * run
                    t0 = scale(x, run, mid, t0)
                    return t0, picked(0, x, run, 8, ny - 8, packed)

                t0, packed = lax.fori_loop(0, piece // run, chunk, (t0, packed))
            zsend[0, h] = packed
            zcopy(0, h).start()

        def step(k, carry):
            if k:
                rims_z(k)

            def windows(h, x, carry):
                for n in range(0, size, window):
                    carry = stencil(k, x + n, window, mid, lambda t: zrecv[k, h, t - 8:t], carry)
                return carry

            carry = inside(k, windows, carry)
            wait_y(k)

            def row_in(x, slot):
                us[k][x + 2, PAD - 2:PAD, :] = yrecv[k, 0, slot]
                if k < 2:
                    us[k][x + 2, PAD + ny:PAD + ny + 2, :] = yrecv[k, 1, slot]

            @pl.loop(0, (nx - 4) // strip)
            def _(i):
                for g in range(strip):
                    row_in(2 + i * strip + g, i * strip + g)

            zcopy(k, 2).wait_recv()

            def border(i, carry):
                return stencil(k, 2 + i * border_run, border_run, ends,
                               lambda t: rrecv[k, 0:8] if t == 0 else rrecv[k, 8:16], carry)

            carry = lax.fori_loop(0, (nx - 4) // border_run, border, carry)
            if k == 1:
                sent(0)
            if k < 2:
                start_y(k + 1)
            wait_x(k)
            for x in (0, 1, nx - 2, nx - 1):
                row_in(x, place(x, True))
            for at in (0, nx - 2):
                carry = stencil(k, at, 2, full, lambda t: rrecv[k, 16 + t:24 + t], carry, True)
            if k < 2:
                start_x(k + 1)
                start_corner(k + 1)
            return carry

        hear(known.at[0], hops[0])
        tell(known.at[1], hops[1])
        s0, s1 = step(0, (zero, zero))
        for n in range(1, len(hops) - 1):
            hear(known.at[n], hops[n])
            tell(known.at[n + 1], hops[n + 1])
        s2, s3 = step(1, (zero, zero))

        owned = nx // ngy
        below = iy == ngy // 2 - 1
        above = iy == ngy // 2

        def fault_copy(which, to):
            return pltpu.make_async_remote_copy(
                fsend.at[:, pl.ds(to * owned, owned), :], frecv.at[which], fs_sem.at[to], fr_sem.at[which],
                device_id=(ix, to, iz), device_id_type=MESH)

        @pl.when(below | above)
        def _():
            edge = jnp.where(below, 1, 0)
            front = jnp.where(below, 1.0 / 24.0, 27.0 / 24.0)
            close = jnp.where(below, -27.0 / 24.0, -1.0 / 24.0)

            def term(x, slot):
                for j in range(3):
                    rows = ysend[j, edge, slot]
                    fsend[j, pl.ds(x, 1), :] = front * rows[0:1] + close * rows[1:2]

            @pl.loop(0, (nx - 4) // strip)
            def _(i):
                for g in range(strip):
                    term(2 + i * strip + g, i * strip + g)

            for x in (0, 1, nx - 2, nx - 1):
                term(x, place(x, True))

        for which, owner in enumerate((ngy // 2 - 1, ngy // 2)):
            @pl.when(iy == owner)
            def _():
                for to in range(ngy):
                    if to != owner:
                        fault_copy(which, to).start()
                frecv[which] = fsend[:, owner * owned:(owner + 1) * owned, :]

        slot = lax.broadcasted_iota(jnp.int32, (1, nz), 1)

        def spread(parts):
            spots = jnp.zeros((1, nz), jnp.float32)
            for j, part, by in parts:
                whole = jnp.sum(jnp.sum(part, axis=0, keepdims=True), axis=1, keepdims=True)
                spots = spots + jnp.where(slot == j, whole * by, 0.0)
            return spots

        unit = 1.0 / 12.0
        early = spread([(0, t0, 1.0), (1, s0, unit), (2, s1, unit), (3, s2, unit), (4, s3, unit)])
        s4 = step(2, zero)
        red[me] = early + spread([(5, s4, unit)])
        hear(known.at[len(hops) - 1], hops[-1])

        def sum_copy(who):
            return pltpu.make_async_remote_copy(
                red.at[me], red.at[me], rs_sem, rr_sem, device_id=who, device_id_type=MESH)

        others = [(x, y, z) for y in reversed(ys) for x in reversed(xs) for z in reversed(zs)][:-1]
        for who in others:
            sum_copy(who).start()

        for which, owner in enumerate((ngy // 2 - 1, ngy // 2)):
            @pl.when(iy != owner)
            def _():
                fault_copy(which, owner).wait_recv()
        sent(1)
        sent(2)
        for which, owner in enumerate((ngy // 2 - 1, ngy // 2)):
            @pl.when(iy == owner)
            def _():
                for to in range(ngy):
                    if to != owner:
                        fault_copy(which, to).wait_send()

        arrived = red.at[pl.ds(0, count - 1)]
        everyone = pltpu.make_async_remote_copy(
            arrived, arrived, rs_sem, rr_sem, device_id=others[0], device_id_type=MESH)
        everyone.wait_recv()
        sums = jnp.sum(red[...], axis=0)
        sums = [jnp.sum(jnp.where(slot == j, sums, 0.0), axis=1, keepdims=True) for j in range(6)]
        coefs = solve(sums[0], sums[1:])
        for j in range(3):
            coef_ref[j:j + 1, :] = jnp.broadcast_to(coefs[j], (1, nz))
        everyone.wait_send()

    return kernel


def blend(u0, u1, u2, coef_ref, fault, pre_ref, state_ref, norm_ref, out, slip, obuf, sbuf, out_sem):
    nx, ny, nz = obuf.shape
    coefs = [coef_ref[j:j + 1, :] for j in range(3)]

    def out_copy(c):
        part = pl.ds(c * CHUNK, CHUNK)
        return pltpu.make_async_copy(obuf.at[part], out.at[part], out_sem.at[c])

    slip_copy = pltpu.make_async_copy(sbuf, slip, out_sem.at[nx // CHUNK])

    def mixed(c):
        @pl.loop(0, CHUNK // 4)
        def _(i):
            for g in range(4):
                x = c * CHUNK + i * 4 + g
                for t in range(PAD, PAD + ny, 8):
                    rows = slice(t, t + 8)
                    obuf[x, t - PAD:t - PAD + 8] = (
                        coefs[0] * u0[x + 2, rows, :] + coefs[1] * u1[x + 2, rows, :]
                        + coefs[2] * u2[x + 2, rows, :])
        out_copy(c).start()

    mixed(0)
    traction = sum(coefs[j] * (fault[0, j] + fault[1, j]) for j in range(3))
    arg = (pre_ref[...] + 2.0 * traction) / norm_ref[...]
    half = jnp.float32(-0.6931471805599453)
    small = arg * (1.0 + arg * arg * (1.0 / 6.0) * (1.0 + arg * arg * 0.05))
    sinh = jnp.where(jnp.abs(arg) < 0.25, small, jnp.exp(arg + half) - jnp.exp(half - arg))
    sbuf[...] = jnp.exp(-state_ref[...]) * sinh
    slip_copy.start()
    pl.loop(1, nx // CHUNK)(mixed)
    slip_copy.wait()
    for c in range(nx // CHUNK):
        out_copy(c).wait()


def solution(mesh):
    sizes = tuple(mesh.shape[a] for a in AXES)
    assert sizes[1] % 2 == 0 and sizes[2] == 2

    def per_device(load, stiffness, prestress, state_var, normal_a):
        nx, ny, nz = load.shape
        assert nx % CHUNK == 0 and nx % 4 == 0 and 2 * nx <= nz and ny % 8 == 0 and ny >= 32
        f32 = jnp.float32
        count = sizes[0] * sizes[1] * sizes[2]
        padded = (nx + 4, ny + 2 * PAD, nz)
        vmem = pl.BlockSpec(memory_space=pltpu.VMEM)
        hbm = pl.BlockSpec(memory_space=pltpu.HBM)
        dma = pltpu.SemaphoreType.DMA
        u0, u1, u2, coefs, fault = pl.pallas_call(
            make_kernel(sizes),
            out_shape=(
                pltpu.VMEM(padded, f32),
                pltpu.VMEM(padded, f32),
                pltpu.VMEM(padded, f32),
                pltpu.VMEM((8, nz), f32),
                pltpu.VMEM((2, 3, nx // sizes[1], nz), f32),
            ),
            in_specs=[hbm, hbm],
            out_specs=(vmem,) * 5,
            scratch_shapes=[
                pltpu.VMEM((nx, ny, nz), f32),
                pltpu.VMEM((nx, ny, nz), f32),
                pltpu.VMEM((3, 2, nx, 2, nz), f32),
                pltpu.VMEM((3, 2, nx, 2, nz), f32),
                pltpu.VMEM((3, 2, ny - 16, nz), f32),
                pltpu.VMEM((3, 2, ny - 16, nz), f32),
                pltpu.VMEM((3, ny + 16, nz), f32),
                pltpu.VMEM((3, ny + 16, nz), f32),
                pltpu.VMEM((2, 2 * nz, 2 * nz), jnp.bfloat16),
                pltpu.VMEM((nx, ny, nz), f32),
                pltpu.VMEM((3, nx, nz), f32),
                pltpu.VMEM((count, 1, nz), f32),
                dma((2 + 2 * LOADS,)),
                dma((2, 6)),
                dma((2, 6)),
                dma((2, 3)),
                dma((2, 3)),
                dma((sizes[1],)),
                dma((2,)),
                dma,
                dma,
                pltpu.SemaphoreType.REGULAR((len(radii(sizes)),)),
            ],
            compiler_params=pltpu.CompilerParams(
                collective_id=0, has_side_effects=True, vmem_limit_bytes=54 * 2**20),
        )(load, stiffness)
        displacement, slip = pl.pallas_call(
            blend,
            out_shape=(
                jax.ShapeDtypeStruct(load.shape, f32),
                jax.ShapeDtypeStruct(prestress.shape, f32),
            ),
            in_specs=[vmem] * 8,
            out_specs=(hbm, hbm),
            scratch_shapes=[
                pltpu.VMEM((nx, ny, nz), f32),
                pltpu.VMEM(prestress.shape, f32),
                dma((nx // CHUNK + 1,)),
            ],
            compiler_params=pltpu.CompilerParams(vmem_limit_bytes=8 * 2**20),
        )(u0, u1, u2, coefs, fault, prestress, state_var, normal_a)
        return displacement, slip

    placed = (
        P("gx", "gy", "gz"),
        P("gx", "gy", "gz"),
        P(("gx", "gy"), "gz"),
        P(("gx", "gy"), "gz"),
        P(("gx", "gy"), "gz"),
    )
    return jax.shard_map(
        per_device,
        mesh=mesh,
        in_specs=placed,
        out_specs=(P("gx", "gy", "gz"), P(("gx", "gy"), "gz")),
        check_vma=False,
    )
```

```python
import jax
import jax.numpy as jnp
from jax import lax
from jax.experimental import pallas as pl
from jax.experimental.pallas import tpu as pltpu
from jax.sharding import PartitionSpec as P

MESH = pl.DeviceIdType.MESH
AXES = ("gx", "gy", "gz")
PAD = 8
CHUNK = 8
PIECES = 4
EARLY = 1


def total(values):
    return jnp.sum(values.reshape(-1, 8, values.shape[-1]), axis=0)


def solve(t0, s):
    t1 = t0 - s[0]
    t2 = t1 - s[1]
    tiny = 1e-7
    p0 = s[0]
    l10 = s[1] / p0
    l20 = s[2] / p0
    p1 = s[2] - l10 * s[1]
    q = s[3] - l20 * s[1]
    ok1 = p1 > tiny * s[2]
    i1 = jnp.where(ok1, 1.0 / jnp.where(ok1, p1, 1.0), 0.0)
    l21 = q * i1
    p2 = s[4] - l20 * s[2] - l21 * q
    ok2 = ok1 & (p2 > tiny * s[4])
    i2 = jnp.where(ok2, 1.0 / jnp.where(ok2, p2, 1.0), 0.0)
    y1 = t1 - l10 * t0
    y2 = t2 - l20 * t0 - l21 * y1
    c2 = y2 * i2
    c1 = y1 * i1 - l21 * c2
    c0 = t0 / p0 - l10 * c1 - l20 * c2
    return c0, c1, c2


def divisor(n, most):
    return max(m for m in range(1, most + 1) if n % m == 0)


def halves(values):
    high = values.astype(jnp.bfloat16)
    return high, (values - high.astype(jnp.float32)).astype(jnp.bfloat16)


def line_rounds(sizes):
    hops = [1]
    while 2 * hops[-1] < max(sizes[:2]) - 1:
        hops.append(2 * hops[-1])
    return hops


def make_kernel(sizes):
    ngx, ngy, ngz = sizes
    count = ngx * ngy * ngz

    def kernel(load, stiff, u0, u1, u2, coef_ref, frecv,
               b, d, ysend, yrecv, zsend, zrecv, rsend, rrecv, band, zterm, fsend, red,
               in_sem, send_sem, x_sem, y_sem, z_sem, fr_sem, rs_sem, rr_sem,
               known):
        nx, ny, nz = b.shape
        us = (u0, u1, u2)
        ix, iy, iz = (lax.axis_index(a) for a in AXES)
        me = (ix * ngy + iy) * ngz + iz
        half = (nx - 4) // 2
        piece = (nx - 4) // PIECES
        window = divisor(piece, 5)
        run_y = divisor(half, 30)
        strip = divisor(half, 6)
        mid = tuple(range(8, ny - 8, 8))
        ends = (0, ny - 8)
        full = tuple(range(0, ny, 8))

        def around(spot, size):
            moved = [spot + n for n in range(size)]
            return [spot] + [jnp.where(m >= size, m - size, m) for m in moved[1:]]

        xs, ys, zs = around(ix, ngx), around(iy, ngy), around(iz, ngz)

        sources = ((load, b), (stiff, d))
        for src, dst in sources:
            for at in (0, nx - 2):
                pltpu.make_async_copy(src.at[at:at + 2], dst.at[at:at + 2], in_sem.at[0]).start()
        for src, dst in sources:
            for at in ends:
                pltpu.make_async_copy(
                    src.at[2:nx - 2, at:at + 8], dst.at[2:nx - 2, at:at + 8], in_sem.at[1]).start()
        for n in range(PIECES):
            part = pl.ds(2 + n * piece, piece)
            for src, dst in sources:
                pltpu.make_async_copy(
                    src.at[part, 8:ny - 8], dst.at[part, 8:ny - 8], in_sem.at[2 + n]).start()

        def loaded(ref, n):
            pltpu.make_async_copy(ref, ref, in_sem.at[n]).wait()

        barrier = pltpu.get_barrier_semaphore()
        def lines(radius, axes=(0, 1)):
            spots = (ix, iy, iz)
            for axis in axes:
                for gap in range(1, min(radius, sizes[axis] - 1) + 1):
                    for step in (-gap, gap):
                        to = spots[axis] + step
                        yield (to >= 0 if step < 0 else to < sizes[axis],
                               tuple(to if n == axis else spot for n, spot in enumerate(spots)))

        def tell(sem, who):
            for there, device in who:
                @pl.when(there)
                def _():
                    pl.semaphore_signal(sem, inc=1, device_id=device, device_id_type=MESH)

        def hear(sem, who):
            pl.semaphore_wait(sem, sum(jnp.where(there, 1, 0) for there, _ in who))

        rounds = ([tuple(lines(hop)) for hop in line_rounds(sizes)]
                  + [tuple(lines(ngy, (1,))), tuple(lines(ngz, (2,)))])
        near = tuple(lines(1, (0, 1, 2)))
        tell(barrier, near)

        zero_plane = jnp.zeros((2, ny, nz), jnp.float32)
        zero_rows = jnp.zeros((nx, 2, nz), jnp.float32)
        for k in range(3):
            @pl.when(ix == 0)
            def _():
                us[k][0:2, PAD:PAD + ny, :] = zero_plane
            @pl.when(ix == ngx - 1)
            def _():
                us[k][nx + 2:nx + 4, PAD:PAD + ny, :] = zero_plane
            @pl.when(iy == 0)
            def _():
                yrecv[k, 0] = zero_rows
            @pl.when(iy == ngy - 1)
            def _():
                yrecv[k, 1] = zero_rows

        row = lax.broadcasted_iota(jnp.int32, (nz, nz), 0)
        col = lax.broadcasted_iota(jnp.int32, (nz, nz), 1)
        far = jnp.bitwise_and(col, 1) + jnp.where(iz == 0, nz, -2)

        def weights(gap, near):
            return jnp.where(near(gap) == 1, 16.0, 0.0) - jnp.where(near(gap) == 2, 1.0, 0.0)

        own = weights(col - row, jnp.abs)
        up = weights(col - row, lambda g: g)
        out = weights(far - row, jnp.abs).astype(jnp.bfloat16)
        for which, part in enumerate((own, up)):
            for n in range(2):
                band[which, n * nz:(n + 1) * nz, 0:nz] = part.astype(jnp.bfloat16)
                band[which, n * nz:(n + 1) * nz, nz:2 * nz] = out

        lane = lax.broadcasted_iota(jnp.int32, (8, nz), 1)
        pair = lane // 2
        edge_low = jnp.where(iz == 0, nz - 2, 0)
        at_edge = (lane >= edge_low) & (lane < edge_low + 2)
        at_upper = at_edge & (iz == 1)

        def xcopy(k, n, side):
            u = us[k]
            rows = pl.ds(PAD + n * (ny // 2), ny // 2)
            if side == 0:
                src, dst, to = u.at[2:4, rows], u.at[nx + 2:nx + 4, rows], ix - 1
            else:
                src, dst, to = u.at[nx:nx + 2, rows], u.at[0:2, rows], ix + 1
            return pltpu.make_async_remote_copy(
                src, dst, send_sem, x_sem.at[k % 2, n, side],
                device_id=(to, iy, iz), device_id_type=MESH)

        def ycopy(k, n, side):
            to = iy - 1 if side == 0 else iy + 1
            part = pl.ds(n * half, half) if n < 2 else pl.ds(nx - 4, 4)
            return pltpu.make_async_remote_copy(
                ysend.at[k, side, part], yrecv.at[k, 1 - side, part], send_sem,
                y_sem.at[k % 2, n, side], device_id=(ix, to, iz), device_id_type=MESH)

        def place(x, rim):
            if not rim:
                return x - 2
            return x if x >= nx - 2 else nx - 4 + x

        def zcopy(k, n):
            rim = isinstance(n, int) and n == PIECES
            src, dst = (rsend.at[k], rrecv.at[k]) if rim else (zsend.at[k, n], zrecv.at[k, n])
            return pltpu.make_async_remote_copy(
                src, dst, send_sem, z_sem.at[k % 2, n],
                device_id=(ix, iy, 1 - iz), device_id_type=MESH)

        def sending(spot, size, side):
            return spot > 0 if side == 0 else spot < size - 1

        def receiving(spot, size, side):
            return spot < size - 1 if side == 0 else spot > 0

        def sides(k):
            return (1,) if k == 2 else (0, 1)

        def each(make, k, n, spot, size, test, act):
            for side in sides(k):
                @pl.when(test(spot, size, side))
                def _():
                    act(make(k, n, side))

        def start_x(k, n, core):
            odd = lax.rem(ix, 2) == 1
            for side, turn in ((1, odd), (0, None), (1, jnp.logical_not(odd))):
                if side in sides(k):
                    go = sending(ix, ngx, side) & (iz == core)
                    @pl.when(go if turn is None else go & turn)
                    def _():
                        xcopy(k, n, side).start()

        def start_y(k, n):
            each(ycopy, k, n, iy, ngy, sending, lambda c: c.start())

        def wait_y(k, n):
            each(ycopy, k, n, iy, ngy, receiving, lambda c: c.wait_recv())

        def wait_x(k, n):
            each(xcopy, k, n, ix, ngx, receiving, lambda c: c.wait_recv())

        def sent(k):
            for n in range(3):
                if n < 2:
                    each(xcopy, k, n, ix, ngx, sending, lambda c: c.wait_send())
                each(ycopy, k, n, iy, ngy, sending, lambda c: c.wait_send())
            for n in range(PIECES + 1):
                zcopy(k, n).wait_send()

        def along_z(k, values, rows):
            high, low = halves(values)
            lhs = jnp.concatenate([high, low], axis=1)
            found = jnp.dot(lhs, band[1 if k == 2 else 0], preferred_element_type=jnp.float32)
            return found[:, :nz].reshape(-1, rows, nz), found[:, nz:].reshape(-1, rows, nz)

        def picked(k, x, n, lo, hi, packed):
            rows = hi - lo
            values = us[k][pl.ds(x + 2, n), PAD + lo:PAD + hi, :].reshape(n * rows, nz)
            own, out = along_z(k, values, rows)
            zterm[pl.ds(x, n), lo:hi, :] = own
            for g in range(n):
                keep = jnp.concatenate([pair] * (rows // 8), axis=0) == x + g
                packed = jnp.where(keep, out[g], packed)
            return packed

        def rims_z(k):
            low = high = jnp.zeros((8, nz), jnp.float32)
            for h in range(2):
                low = picked(k, 2 + h * half, half, 0, 8, low)
                high = picked(k, 2 + h * half, half, ny - 8, ny, high)
            rsend[k, 0:8] = low
            rsend[k, 8:16] = high
            packed = jnp.zeros((ny, nz), jnp.float32)
            for at in (0, nx - 2):
                packed = picked(k, at, 2, 0, ny, packed)
            rsend[k, 16:16 + ny] = packed
            zcopy(k, PIECES).start()

        def put(k, x, slot, t, value):
            us[k][x + 2, PAD + t:PAD + t + 8, :] = value
            if t == 0:
                ysend[k, 0, slot] = value[0:2]
            if t == ny - 8:
                ysend[k, 1, slot] = value[6:8]

        def scale(x, n, tiles, t0, slot=None):
            for g in range(n):
                for t in tiles:
                    rows = slice(t, t + 8)
                    inv = 1.0 / (7.5 + d[x + g, rows])
                    rhs = b[x + g, rows]
                    value = inv * rhs
                    d[x + g, rows] = inv * (1.0 / 12.0)
                    b[x + g, rows] = 12.0 * rhs
                    put(0, x + g, x + g - 2 if slot is None else slot, t, value)
                    t0 = t0 + value * rhs
            return t0

        def shift_of(x):
            return jnp.bitwise_and(jnp.where(iz == 0, nz - 2, nz) - 2 * x, nz - 1)

        def stencil(k, x, n, tiles, source, carry, rim=False):
            u = us[k]
            for t in tiles:
                lo, hi = PAD + t, PAD + t + 8
                packed = source(t)
                line = [u[x + j, lo:hi, :] for j in range(n + 4 if k < 2 else n + 2)]
                for g in range(n):
                    at = x + g
                    rows = slice(t, t + 8)
                    c = line[g + 2]
                    z = zterm[at, rows] + jnp.where(
                        at_edge if k < 2 else at_upper, pltpu.roll(packed, shift_of(at), 1), 0.0)
                    if k < 2:
                        even, odd = carry
                        one = ((line[g + 1] + line[g + 3])
                               + (u[at + 2, lo - 1:hi - 1, :] + u[at + 2, lo + 1:hi + 1, :]))
                        two = ((line[g] + line[g + 4])
                               + (u[at + 2, lo - 2:hi - 2, :] + u[at + 2, lo + 2:hi + 2, :]))
                        w = (16.0 * one - two) + z
                        fresh = d[at, rows] * w
                        even = even + c * (b[at, rows] - w)
                        odd = odd + (c - fresh) * w
                        b[at, rows] = w
                        put(k + 1, at, place(at, rim), t, fresh)
                        carry = even, odd
                    else:
                        one = line[g + 1] + u[at + 2, lo - 1:hi - 1, :]
                        two = line[g] + u[at + 2, lo - 2:hi - 2, :]
                        w = (16.0 * one - two) + z
                        carry = carry + c * (b[at, rows] - (w + w))
            return carry

        def pack(k, n):
            packed = picked(k, 2 + n * piece, piece, 8, ny - 8, jnp.zeros((ny - 16, nz), jnp.float32))
            zsend[k, n] = packed
            zcopy(k, n).start()

        def inside(k, first, last, carry):
            def part(n, carry):
                zcopy(k, n).wait_recv()
                x = 2 + n * piece
                for g in range(0, piece, window):
                    carry = stencil(k, x + g, window, mid, lambda t: zrecv[k, n, t - 8:t], carry)
                if k < 2:
                    pack(k + 1, n)
                return carry

            return lax.fori_loop(first, last, part, carry)

        zero = jnp.zeros((8, nz), jnp.float32)

        loaded(b.at[0:8], 0)
        t0 = lax.fori_loop(0, 4, lambda n, c: scale(
            jnp.where(n < 2, n, nx - 4 + n), 1, full, c, nx - 4 + n), zero)
        loaded(b.at[2:nx - 2, 0:32], 1)
        for h in range(2):
            t0 = lax.fori_loop(
                0, half // strip, lambda n, c: scale(2 + h * half + n * strip, strip, ends, c), t0)
            if h == 0:
                hear(barrier, near)
                for n in range(2):
                    start_x(0, n, 0)
                    start_x(0, n, 1)
            start_y(0, h)
        start_y(0, 2)
        tell(known.at[0], rounds[0])
        rims_z(0)

        def fresh_part(n, t0):
            loaded(b.at[0:2 * piece, 8:ny - 8], 2 + n)
            t0 = scale(2 + n * piece, piece, mid, t0)
            pack(0, n)
            return t0

        def late_x(k):
            for n in range(2):
                start_x(k, n, 1)

        t0 = lax.fori_loop(0, PIECES, fresh_part, t0)

        def row_in(k, x, slot, side_set):
            if 0 in side_set:
                us[k][x + 2, PAD - 2:PAD, :] = yrecv[k, 0, slot]
            if 1 in side_set and k < 2:
                us[k][x + 2, PAD + ny:PAD + ny + 2, :] = yrecv[k, 1, slot]

        def border(k, h, carry):
            wait_y(k, h)

            @pl.loop(0, half // strip)
            def _(i):
                for g in range(strip):
                    slot = h * half + i * strip + g
                    row_in(k, slot + 2, slot, (0, 1))

            def piece_of(i, carry):
                return stencil(k, 2 + h * half + i * run_y, run_y, ends,
                               lambda t: rrecv[k, 0:8] if t == 0 else rrecv[k, 8:16], carry)

            carry = lax.fori_loop(0, half // run_y, piece_of, carry)
            if k < 2:
                start_y(k + 1, h)
            return carry

        def outer(k, n, carry):
            wait_x(k, n)
            for x in (0, 1, nx - 2, nx - 1):
                row_in(k, x, place(x, True), (n,))
            for at in (0, nx - 2):
                carry = stencil(k, at, 2, full[n * len(full) // 2:(n + 1) * len(full) // 2],
                                lambda t: rrecv[k, 16 + t:24 + t], carry, True)
            if k < 2:
                start_x(k + 1, n, 0)
                if k == 1:
                    start_x(k + 1, n, 1)
            return carry

        def borders(k, carry):
            zcopy(k, PIECES).wait_recv()
            for h in range(2):
                carry = border(k, h, carry)
            wait_y(k, 2)
            return carry

        def pass_on(n):
            hear(known.at[n], rounds[n])
            if n + 1 < len(rounds):
                tell(known.at[n + 1], rounds[n + 1])

        lead = PIECES - 1
        state = inside(0, 0, lead, (zero, zero))
        for n in range(len(rounds) - 3):
            pass_on(n)
        state = borders(0, state)
        state = outer(0, 1, outer(0, 0, state))
        start_y(1, 2)
        s0, s1 = inside(0, lead, PIECES, state)
        late_x(1)
        rims_z(1)
        state = inside(1, 0, lead, (zero, zero))
        pass_on(len(rounds) - 3)
        state = borders(1, state)
        state = outer(1, 0, state)
        state = inside(1, lead, PIECES, state)
        s2, s3 = outer(1, 1, state)
        start_y(2, 2)
        rims_z(2)

        owned = nx // ngy
        below = iy == ngy // 2 - 1
        above = iy == ngy // 2

        def fault_copy(which, to):
            return pltpu.make_async_remote_copy(
                fsend.at[:, pl.ds(to * owned, owned), :], frecv.at[which], send_sem, fr_sem.at[which],
                device_id=(ix, to, iz), device_id_type=MESH)

        @pl.when(below | above)
        def _():
            edge = jnp.where(below, 1, 0)
            front = jnp.where(below, 1.0 / 24.0, 27.0 / 24.0)
            close = jnp.where(below, -27.0 / 24.0, -1.0 / 24.0)

            def term(x, slot):
                for j in range(3):
                    rows = ysend[j, edge, slot]
                    fsend[j, pl.ds(x, 1), :] = front * rows[0:1] + close * rows[1:2]

            @pl.loop(0, (nx - 4) // strip)
            def _(i):
                for g in range(strip):
                    term(2 + i * strip + g, i * strip + g)

            for x in (0, 1, nx - 2, nx - 1):
                term(x, place(x, True))

        for which, owner in enumerate((ngy // 2 - 1, ngy // 2)):
            @pl.when(iy == owner)
            def _():
                for to in range(ngy):
                    if to != owner:
                        fault_copy(which, to).start()
                frecv[which] = fsend[:, owner * owned:(owner + 1) * owned, :]

        slot = lax.broadcasted_iota(jnp.int32, (1, nz), 1)

        def spread(parts):
            spots = jnp.zeros((1, nz), jnp.float32)
            for j, part, by in parts:
                whole = jnp.sum(jnp.sum(part, axis=0, keepdims=True), axis=1, keepdims=True)
                spots = spots + jnp.where(slot == j, whole * by, 0.0)
            return spots

        unit = 1.0 / 12.0
        early = spread([(0, t0, 1.0), (1, s0, unit), (2, s1, unit), (3, s2, unit), (4, s3, unit)])
        s4 = inside(2, 0, PIECES, zero)
        s4 = borders(2, s4)
        pass_on(len(rounds) - 2)
        s4 = outer(2, 1, outer(2, 0, s4))
        red[me] = early + spread([(5, s4, unit)])
        hear(known.at[len(rounds) - 1], rounds[-1])

        def sum_copy(who):
            return pltpu.make_async_remote_copy(
                red.at[me], red.at[me], rs_sem, rr_sem, device_id=who, device_id_type=MESH)

        others = [(x, y, z) for y in reversed(ys) for x in reversed(xs) for z in reversed(zs)][:-1]
        for who in others:
            sum_copy(who).start()

        for which, owner in enumerate((ngy // 2 - 1, ngy // 2)):
            @pl.when(iy != owner)
            def _():
                fault_copy(which, owner).wait_recv()
        for k in range(3):
            sent(k)
        for which, owner in enumerate((ngy // 2 - 1, ngy // 2)):
            @pl.when(iy == owner)
            def _():
                for to in range(ngy):
                    if to != owner:
                        fault_copy(which, to).wait_send()

        arrived = red.at[pl.ds(0, count - 1)]
        everyone = pltpu.make_async_remote_copy(
            arrived, arrived, rs_sem, rr_sem, device_id=others[0], device_id_type=MESH)
        everyone.wait_recv()
        sums = jnp.sum(red[...], axis=0)
        sums = [jnp.sum(jnp.where(slot == j, sums, 0.0), axis=1, keepdims=True) for j in range(6)]
        coefs = solve(sums[0], sums[1:])
        for j in range(3):
            coef_ref[j:j + 1, :] = jnp.broadcast_to(coefs[j], (1, nz))
        everyone.wait_send()

    return kernel


def blend(u0, u1, u2, coef_ref, fault, pre_ref, state_ref, norm_ref, out, slip, obuf, sbuf, out_sem):
    nx, ny, nz = obuf.shape
    coefs = [coef_ref[j:j + 1, :] for j in range(3)]

    def out_copy(c):
        part = pl.ds(c * CHUNK, CHUNK)
        return pltpu.make_async_copy(obuf.at[part], out.at[part], out_sem.at[c])

    slip_copy = pltpu.make_async_copy(sbuf, slip, out_sem.at[nx // CHUNK])

    def mixed(c):
        @pl.loop(0, CHUNK // 4)
        def _(i):
            for g in range(4):
                x = c * CHUNK + i * 4 + g
                for t in range(PAD, PAD + ny, 8):
                    rows = slice(t, t + 8)
                    obuf[x, t - PAD:t - PAD + 8] = (
                        coefs[0] * u0[x + 2, rows, :] + coefs[1] * u1[x + 2, rows, :]
                        + coefs[2] * u2[x + 2, rows, :])
        out_copy(c).start()

    mixed(0)
    traction = sum(coefs[j] * (fault[0, j] + fault[1, j]) for j in range(3))
    arg = (pre_ref[...] + 2.0 * traction) / norm_ref[...]
    half = jnp.float32(-0.6931471805599453)
    small = arg * (1.0 + arg * arg * (1.0 / 6.0) * (1.0 + arg * arg * 0.05))
    sinh = jnp.where(jnp.abs(arg) < 0.25, small, jnp.exp(arg + half) - jnp.exp(half - arg))
    sbuf[...] = jnp.exp(-state_ref[...]) * sinh
    slip_copy.start()
    pl.loop(1, nx // CHUNK)(mixed)
    slip_copy.wait()
    for c in range(nx // CHUNK):
        out_copy(c).wait()


def solution(mesh):
    sizes = tuple(mesh.shape[a] for a in AXES)
    assert sizes[1] % 2 == 0 and sizes[2] == 2

    def per_device(load, stiffness, prestress, state_var, normal_a):
        nx, ny, nz = load.shape
        assert nx % CHUNK == 0 and nx % 4 == 0 and 2 * nx <= nz and (nx - 4) % PIECES == 0 and ny % 8 == 0 and ny >= 32
        f32 = jnp.float32
        count = sizes[0] * sizes[1] * sizes[2]
        padded = (nx + 4, ny + 2 * PAD, nz)
        vmem = pl.BlockSpec(memory_space=pltpu.VMEM)
        hbm = pl.BlockSpec(memory_space=pltpu.HBM)
        dma = pltpu.SemaphoreType.DMA
        u0, u1, u2, coefs, fault = pl.pallas_call(
            make_kernel(sizes),
            out_shape=(
                pltpu.VMEM(padded, f32),
                pltpu.VMEM(padded, f32),
                pltpu.VMEM(padded, f32),
                pltpu.VMEM((8, nz), f32),
                pltpu.VMEM((2, 3, nx // sizes[1], nz), f32),
            ),
            in_specs=[hbm, hbm],
            out_specs=(vmem,) * 5,
            scratch_shapes=[
                pltpu.VMEM((nx, ny, nz), f32),
                pltpu.VMEM((nx, ny, nz), f32),
                pltpu.VMEM((3, 2, nx, 2, nz), f32),
                pltpu.VMEM((3, 2, nx, 2, nz), f32),
                pltpu.VMEM((3, PIECES, ny - 16, nz), f32),
                pltpu.VMEM((3, PIECES, ny - 16, nz), f32),
                pltpu.VMEM((3, ny + 16, nz), f32),
                pltpu.VMEM((3, ny + 16, nz), f32),
                pltpu.VMEM((2, 2 * nz, 2 * nz), jnp.bfloat16),
                pltpu.VMEM((nx, ny, nz), f32),
                pltpu.VMEM((3, nx, nz), f32),
                pltpu.VMEM((count, 1, nz), f32),
                dma((2 + PIECES,)),
                dma,
                dma((2, 2, 2)),
                dma((2, 3, 2)),
                dma((2, PIECES + 1)),
                dma((2,)),
                dma,
                dma,
                pltpu.SemaphoreType.REGULAR((len(line_rounds(sizes)) + 2,)),
            ],
            compiler_params=pltpu.CompilerParams(
                collective_id=0, has_side_effects=True, vmem_limit_bytes=54 * 2**20),
        )(load, stiffness)
        displacement, slip = pl.pallas_call(
            blend,
            out_shape=(
                jax.ShapeDtypeStruct(load.shape, f32),
                jax.ShapeDtypeStruct(prestress.shape, f32),
            ),
            in_specs=[vmem] * 8,
            out_specs=(hbm, hbm),
            scratch_shapes=[
                pltpu.VMEM((nx, ny, nz), f32),
                pltpu.VMEM(prestress.shape, f32),
                dma((nx // CHUNK + 1,)),
            ],
            compiler_params=pltpu.CompilerParams(vmem_limit_bytes=8 * 2**20),
        )(u0, u1, u2, coefs, fault, prestress, state_var, normal_a)
        return displacement, slip

    placed = (
        P("gx", "gy", "gz"),
        P("gx", "gy", "gz"),
        P(("gx", "gy"), "gz"),
        P(("gx", "gy"), "gz"),
        P(("gx", "gy"), "gz"),
    )
    return jax.shard_map(
        per_device,
        mesh=mesh,
        in_specs=placed,
        out_specs=(P("gx", "gy", "gz"), P(("gx", "gy"), "gz")),
        check_vma=False,
    )
```

```python
import jax
import jax.numpy as jnp
from jax import lax
from jax.experimental import pallas as pl
from jax.experimental.pallas import tpu as pltpu
from jax.sharding import PartitionSpec as P

MESH = pl.DeviceIdType.MESH
AXES = ("gx", "gy", "gz")
PAD = 8
CHUNK = 8
PIECES = 4


def total(values):
    return jnp.sum(values.reshape(-1, 8, values.shape[-1]), axis=0)


def solve(t0, s):
    t1 = t0 - s[0]
    t2 = t1 - s[1]
    tiny = 1e-7
    p0 = s[0]
    l10 = s[1] / p0
    l20 = s[2] / p0
    p1 = s[2] - l10 * s[1]
    q = s[3] - l20 * s[1]
    ok1 = p1 > tiny * s[2]
    i1 = jnp.where(ok1, 1.0 / jnp.where(ok1, p1, 1.0), 0.0)
    l21 = q * i1
    p2 = s[4] - l20 * s[2] - l21 * q
    ok2 = ok1 & (p2 > tiny * s[4])
    i2 = jnp.where(ok2, 1.0 / jnp.where(ok2, p2, 1.0), 0.0)
    y1 = t1 - l10 * t0
    y2 = t2 - l20 * t0 - l21 * y1
    c2 = y2 * i2
    c1 = y1 * i1 - l21 * c2
    c0 = t0 / p0 - l10 * c1 - l20 * c2
    return c0, c1, c2


def divisor(n, most):
    return max(m for m in range(1, most + 1) if n % m == 0)


def halves(values):
    high = values.astype(jnp.bfloat16)
    return high, (values - high.astype(jnp.float32)).astype(jnp.bfloat16)


def line_rounds(sizes):
    hops = [1]
    while 2 * hops[-1] < max(sizes[:2]) - 1:
        hops.append(2 * hops[-1])
    return hops


def make_kernel(sizes):
    ngx, ngy, ngz = sizes
    count = ngx * ngy * ngz

    def kernel(load, stiff, u0, u1, u2, coef_ref, frecv,
               b, d, ysend, yrecv, zsend, zrecv, rsend, rrecv, band, zterm, fsend, red,
               dhalo, qsend, qhalo,
               in_sem, send_sem, x_sem, y_sem, z_sem, fr_sem, rs_sem, rr_sem, q_sem,
               known):
        nx, ny, nz = b.shape
        us = (u0, u1, u2)
        ix, iy, iz = (lax.axis_index(a) for a in AXES)
        me = (ix * ngy + iy) * ngz + iz
        half = (nx - 4) // 2
        piece = (nx - 4) // PIECES
        window = divisor(piece, 5)
        run_y = divisor(half, 30)
        strip = divisor(half, 6)
        mid = tuple(range(8, ny - 8, 8))
        ends = (0, ny - 8)
        full = tuple(range(0, ny, 8))

        def around(spot, size):
            moved = [spot + n for n in range(size)]
            return [spot] + [jnp.where(m >= size, m - size, m) for m in moved[1:]]

        xs, ys, zs = around(ix, ngx), around(iy, ngy), around(iz, ngz)

        sources = ((load, b), (stiff, d))
        for src, dst in sources:
            for at in (0, nx - 2):
                pltpu.make_async_copy(src.at[at:at + 2], dst.at[at:at + 2], in_sem.at[0]).start()
        for src, dst in sources:
            for at in ends:
                pltpu.make_async_copy(
                    src.at[2:nx - 2, at:at + 8], dst.at[2:nx - 2, at:at + 8], in_sem.at[1]).start()
        for n in range(PIECES):
            part = pl.ds(2 + n * piece, piece)
            for src, dst in sources:
                pltpu.make_async_copy(
                    src.at[part, 8:ny - 8], dst.at[part, 8:ny - 8], in_sem.at[2 + n]).start()

        def loaded(ref, n):
            pltpu.make_async_copy(ref, ref, in_sem.at[n]).wait()

        barrier = pltpu.get_barrier_semaphore()
        def lines(radius, axes=(0, 1)):
            spots = (ix, iy, iz)
            for axis in axes:
                for gap in range(1, min(radius, sizes[axis] - 1) + 1):
                    for step in (-gap, gap):
                        to = spots[axis] + step
                        yield (to >= 0 if step < 0 else to < sizes[axis],
                               tuple(to if n == axis else spot for n, spot in enumerate(spots)))

        def tell(sem, who):
            for there, device in who:
                @pl.when(there)
                def _():
                    pl.semaphore_signal(sem, inc=1, device_id=device, device_id_type=MESH)

        def hear(sem, who):
            pl.semaphore_wait(sem, sum(jnp.where(there, 1, 0) for there, _ in who))

        rounds = ([tuple(lines(hop)) for hop in line_rounds(sizes)]
                  + [tuple(lines(ngy, (1,))), tuple(lines(ngz, (2,)))])
        near = tuple(lines(1, (0, 1, 2)))
        tell(barrier, near)

        zero_plane = jnp.zeros((2, ny, nz), jnp.float32)
        zero_rows = jnp.zeros((nx, 2, nz), jnp.float32)
        for k in range(3):
            @pl.when(ix == 0)
            def _():
                us[k][0:2, PAD:PAD + ny, :] = zero_plane
            @pl.when(ix == ngx - 1)
            def _():
                us[k][nx + 2:nx + 4, PAD:PAD + ny, :] = zero_plane
            @pl.when(iy == 0)
            def _():
                yrecv[k, 0] = zero_rows
            @pl.when(iy == ngy - 1)
            def _():
                yrecv[k, 1] = zero_rows

        row = lax.broadcasted_iota(jnp.int32, (nz, nz), 0)
        col = lax.broadcasted_iota(jnp.int32, (nz, nz), 1)
        far = jnp.bitwise_and(col, 1) + jnp.where(iz == 0, nz, -2)

        def weights(gap, near):
            return jnp.where(near(gap) == 1, 16.0, 0.0) - jnp.where(near(gap) == 2, 1.0, 0.0)

        own = weights(col - row, jnp.abs)
        up = weights(col - row, lambda g: g)
        out = weights(far - row, jnp.abs).astype(jnp.bfloat16)
        for which, part in enumerate((own, up)):
            for n in range(2):
                band[which, n * nz:(n + 1) * nz, 0:nz] = part.astype(jnp.bfloat16)
                band[which, n * nz:(n + 1) * nz, nz:2 * nz] = out

        lane = lax.broadcasted_iota(jnp.int32, (8, nz), 1)
        pair = lane // 2
        edge_low = jnp.where(iz == 0, nz - 2, 0)
        at_edge = (lane >= edge_low) & (lane < edge_low + 2)
        at_upper = at_edge & (iz == 1)

        def xcopy(k, side):
            u = us[k]
            rows = pl.ds(PAD, ny)
            if side == 0:
                src, dst, to = u.at[2:4, rows], u.at[nx + 2:nx + 4, rows], ix - 1
            else:
                src, dst, to = u.at[nx:nx + 2, rows], u.at[0:2, rows], ix + 1
            return pltpu.make_async_remote_copy(
                src, dst, send_sem, x_sem.at[k, side],
                device_id=(to, iy, iz), device_id_type=MESH)

        def ycopy(k, n, side):
            to = iy - 1 if side == 0 else iy + 1
            part = pl.ds(n * half, half) if n < 2 else pl.ds(nx - 4, 4)
            return pltpu.make_async_remote_copy(
                ysend.at[k, side, part], yrecv.at[k, 1 - side, part], send_sem,
                y_sem.at[k % 2, n, side], device_id=(ix, to, iz), device_id_type=MESH)

        def place(x, rim):
            if not rim:
                return x - 2
            return x if x >= nx - 2 else nx - 4 + x

        def zcopy(k, n):
            rim = isinstance(n, int) and n == PIECES
            src, dst = (rsend.at[k], rrecv.at[k]) if rim else (zsend.at[k, n], zrecv.at[k, n])
            return pltpu.make_async_remote_copy(
                src, dst, send_sem, z_sem.at[k % 2, n],
                device_id=(ix, iy, 1 - iz), device_id_type=MESH)

        def sending(spot, size, side):
            return spot > 0 if side == 0 else spot < size - 1

        def receiving(spot, size, side):
            return spot < size - 1 if side == 0 else spot > 0

        def sides(k):
            return (0,) if k == 2 else (0, 1)

        def d_copy():
            return pltpu.make_async_remote_copy(
                d.at[nx - 2:nx], dhalo, send_sem, q_sem.at[0],
                device_id=(ix + 1, iy, iz), device_id_type=MESH)

        def q_copy():
            return pltpu.make_async_remote_copy(
                qsend, qhalo, send_sem, q_sem.at[1],
                device_id=(ix + 1, iy, iz), device_id_type=MESH)

        def each(make, k, n, spot, size, test, act):
            for side in sides(k):
                @pl.when(test(spot, size, side))
                def _():
                    act(make(k, n, side))

        def start_x(k):
            odd = lax.rem(ix, 2) == 1
            for side, turn in ((1, odd), (0, None), (1, jnp.logical_not(odd))):
                go = sending(ix, ngx, side)
                @pl.when(go if turn is None else go & turn)
                def _():
                    xcopy(k, side).start()

        def start_y(k, n):
            each(ycopy, k, n, iy, ngy, sending, lambda c: c.start())

        def wait_y(k, n):
            each(ycopy, k, n, iy, ngy, receiving, lambda c: c.wait_recv())

        def wait_x(k, n=0):
            each(lambda k, n, side: xcopy(k, side), k, n, ix, ngx, receiving, lambda c: c.wait_recv())

        def sent(k):
            for n in range(3):
                if n == 0 and k < 2:
                    each(lambda k, n, side: xcopy(k, side), k, n, ix, ngx, sending, lambda c: c.wait_send())
                each(ycopy, k, n, iy, ngy, sending, lambda c: c.wait_send())
            for n in range(PIECES + 1):
                zcopy(k, n).wait_send()

        def along_z(k, values, rows):
            high, low = halves(values)
            lhs = jnp.concatenate([high, low], axis=1)
            found = jnp.dot(lhs, band[1 if k == 2 else 0], preferred_element_type=jnp.float32)
            return found[:, :nz].reshape(-1, rows, nz), found[:, nz:].reshape(-1, rows, nz)

        def picked(k, x, n, lo, hi, packed):
            rows = hi - lo
            values = us[k][pl.ds(x + 2, n), PAD + lo:PAD + hi, :].reshape(n * rows, nz)
            own, out = along_z(k, values, rows)
            zterm[pl.ds(x, n), lo:hi, :] = own
            for g in range(n):
                keep = jnp.concatenate([pair] * (rows // 8), axis=0) == x + g
                packed = jnp.where(keep, out[g], packed)
            return packed

        def rims_z(k):
            low = high = jnp.zeros((8, nz), jnp.float32)
            for h in range(2):
                low = picked(k, 2 + h * half, half, 0, 8, low)
                high = picked(k, 2 + h * half, half, ny - 8, ny, high)
            rsend[k, 0:8] = low
            rsend[k, 8:16] = high
            packed = jnp.zeros((ny, nz), jnp.float32)
            for at in (0, nx - 2):
                packed = picked(k, at, 2, 0, ny, packed)
            rsend[k, 16:16 + ny] = packed
            zcopy(k, PIECES).start()

        def put(k, x, slot, t, value):
            us[k][x + 2, PAD + t:PAD + t + 8, :] = value
            if t == 0:
                ysend[k, 0, slot] = value[0:2]
            if t == ny - 8:
                ysend[k, 1, slot] = value[6:8]

        def scale(x, n, tiles, t0, slot=None):
            for g in range(n):
                for t in tiles:
                    rows = slice(t, t + 8)
                    inv = 1.0 / (7.5 + d[x + g, rows])
                    rhs = b[x + g, rows]
                    value = inv * rhs
                    d[x + g, rows] = inv * (1.0 / 12.0)
                    b[x + g, rows] = 12.0 * rhs
                    put(0, x + g, x + g - 2 if slot is None else slot, t, value)
                    t0 = t0 + value * rhs
            return t0

        def shift_of(x):
            return jnp.bitwise_and(jnp.where(iz == 0, nz - 2, nz) - 2 * x, nz - 1)

        def stencil(k, x, n, tiles, source, carry, rim=False):
            u = us[k]
            for t in tiles:
                lo, hi = PAD + t, PAD + t + 8
                packed = source(t)
                line = [u[x + j, lo:hi, :] for j in range(n + 4 if k < 2 else n + 2)]
                for g in range(n):
                    at = x + g
                    rows = slice(t, t + 8)
                    c = line[g + 2]
                    z = zterm[at, rows] + jnp.where(
                        at_edge if k < 2 else at_upper, pltpu.roll(packed, shift_of(at), 1), 0.0)
                    if k < 2:
                        even, odd = carry
                        one = ((line[g + 1] + line[g + 3])
                               + (u[at + 2, lo - 1:hi - 1, :] + u[at + 2, lo + 1:hi + 1, :]))
                        two = ((line[g] + line[g + 4])
                               + (u[at + 2, lo - 2:hi - 2, :] + u[at + 2, lo + 2:hi + 2, :]))
                        w = (16.0 * one - two) + z
                        fresh = d[at, rows] * w
                        even = even + c * (b[at, rows] - w)
                        odd = odd + (c - fresh) * w
                        b[at, rows] = w
                        put(k + 1, at, place(at, rim), t, fresh)
                        carry = even, odd
                    else:
                        one = line[g + 1] + u[at + 2, lo + 1:hi + 1, :]
                        two = line[g] + u[at + 2, lo + 2:hi + 2, :]
                        w = (16.0 * one - two) + z
                        carry = carry + c * (b[at, rows] - (w + w))
            return carry

        def pack(k, n):
            packed = picked(k, 2 + n * piece, piece, 8, ny - 8, jnp.zeros((ny - 16, nz), jnp.float32))
            zsend[k, n] = packed
            zcopy(k, n).start()

        def inside(k, first, last, carry):
            def part(n, carry):
                zcopy(k, n).wait_recv()
                x = 2 + n * piece
                for g in range(0, piece, window):
                    carry = stencil(k, x + g, window, mid, lambda t: zrecv[k, n, t - 8:t], carry)
                if k < 2:
                    pack(k + 1, n)
                return carry

            return lax.fori_loop(first, last, part, carry)

        zero = jnp.zeros((8, nz), jnp.float32)

        loaded(b.at[0:8], 0)
        t0 = lax.fori_loop(0, 4, lambda n, c: scale(
            jnp.where(n < 2, n, nx - 4 + n), 1, full, c, nx - 4 + n), zero)
        loaded(b.at[2:nx - 2, 0:32], 1)
        for h in range(2):
            t0 = lax.fori_loop(
                0, half // strip, lambda n, c: scale(2 + h * half + n * strip, strip, ends, c), t0)
            if h == 0:
                hear(barrier, near)
                start_x(0)
            start_y(0, h)
        start_y(0, 2)
        tell(known.at[0], rounds[0])
        rims_z(0)

        def fresh_part(n, t0):
            loaded(b.at[0:2 * piece, 8:ny - 8], 2 + n)
            t0 = scale(2 + n * piece, piece, mid, t0)
            pack(0, n)
            return t0

        t0 = lax.fori_loop(0, PIECES, fresh_part, t0)

        def row_in(k, x, slot, side_set):
            if 0 in side_set and k < 2:
                us[k][x + 2, PAD - 2:PAD, :] = yrecv[k, 0, slot]
            if 1 in side_set:
                us[k][x + 2, PAD + ny:PAD + ny + 2, :] = yrecv[k, 1, slot]

        def border(k, h, carry):
            wait_y(k, h)

            @pl.loop(0, half // strip)
            def _(i):
                for g in range(strip):
                    slot = h * half + i * strip + g
                    row_in(k, slot + 2, slot, (0, 1))

            def piece_of(i, carry):
                return stencil(k, 2 + h * half + i * run_y, run_y, ends,
                               lambda t: rrecv[k, 0:8] if t == 0 else rrecv[k, 8:16], carry)

            carry = lax.fori_loop(0, half // run_y, piece_of, carry)
            if k < 2:
                start_y(k + 1, h)
            return carry

        def outer(k, n, carry):
            for x in (0, 1, nx - 2, nx - 1):
                row_in(k, x, place(x, True), (n,))
            for at in (0, nx - 2):
                carry = stencil(k, at, 2, full[n * len(full) // 2:(n + 1) * len(full) // 2],
                                lambda t: rrecv[k, 16 + t:24 + t], carry, True)
            return carry

        def lacking():
            for x in (0, 1, nx - 2, nx - 1):
                row_in(1, x, place(x, True), (0, 1))

            @pl.when(ix < ngx - 1)
            def _():
                at = nx - 2
                for t in full:
                    lo, hi = PAD + t, PAD + t + 8
                    line = [u1[at + j, lo:hi, :] for j in range(4)]
                    for g in range(2):
                        z = zterm[at + g, t:t + 8] + jnp.where(
                            at_edge, pltpu.roll(rrecv[1, 16 + t:24 + t], shift_of(at + g), 1), 0.0)
                        one = line[g + 1] + (u1[at + g + 2, lo - 1:hi - 1, :] + u1[at + g + 2, lo + 1:hi + 1, :])
                        two = line[g] + (u1[at + g + 2, lo - 2:hi - 2, :] + u1[at + g + 2, lo + 2:hi + 2, :])
                        if g == 0:
                            one = one + line[3]
                        qsend[g, t:t + 8] = (16.0 * one - two) + z
                q_copy().start()

        def last_planes(carry):
            for x in (0, 1, nx - 2, nx - 1):
                row_in(2, x, place(x, True), (1,))
            carry = stencil(2, nx - 2, 2, full, lambda t: rrecv[2, 16 + t:24 + t], carry, True)

            @pl.when(ix > 0)
            def _():
                d_copy().wait_recv()
                q_copy().wait_recv()
                for t in full:
                    rows, lines = slice(t, t + 8), slice(PAD + t, PAD + t + 8)
                    first, second = u1[2, lines, :], u1[3, lines, :]
                    u2[1, lines, :] = dhalo[1, rows] * (qhalo[1, rows] + (16.0 * first - second))
                    u2[0, lines, :] = dhalo[0, rows] * (qhalo[0, rows] - first)

            return stencil(2, 0, 2, full, lambda t: rrecv[2, 16 + t:24 + t], carry, True)

        def borders(k, carry):
            zcopy(k, PIECES).wait_recv()
            for h in range(2):
                carry = border(k, h, carry)
            wait_y(k, 2)
            return carry

        def pass_on(n):
            hear(known.at[n], rounds[n])
            if n + 1 < len(rounds):
                tell(known.at[n + 1], rounds[n + 1])

        @pl.when(ix < ngx - 1)
        def _():
            d_copy().start()

        lead = PIECES - 1
        state = inside(0, 0, lead, (zero, zero))
        for n in range(len(rounds) - 3):
            pass_on(n)
        state = borders(0, state)
        wait_x(0)
        state = outer(0, 1, outer(0, 0, state))
        start_x(1)
        start_y(1, 2)
        s0, s1 = inside(0, lead, PIECES, state)
        rims_z(1)
        state = inside(1, 0, lead, (zero, zero))
        pass_on(len(rounds) - 3)
        state = borders(1, state)
        lacking()
        state = inside(1, lead, PIECES, state)
        wait_x(1)
        state = outer(1, 0, state)
        start_y(2, 2)
        s2, s3 = outer(1, 1, state)
        rims_z(2)

        owned = nx // ngy
        below = iy == ngy // 2 - 1
        above = iy == ngy // 2

        def fault_copy(which, to):
            return pltpu.make_async_remote_copy(
                fsend.at[:, pl.ds(to * owned, owned), :], frecv.at[which], send_sem, fr_sem.at[which],
                device_id=(ix, to, iz), device_id_type=MESH)

        @pl.when(below | above)
        def _():
            edge = jnp.where(below, 1, 0)
            front = jnp.where(below, 1.0 / 24.0, 27.0 / 24.0)
            close = jnp.where(below, -27.0 / 24.0, -1.0 / 24.0)

            def term(x, slot):
                for j in range(3):
                    rows = ysend[j, edge, slot]
                    fsend[j, pl.ds(x, 1), :] = front * rows[0:1] + close * rows[1:2]

            @pl.loop(0, (nx - 4) // strip)
            def _(i):
                for g in range(strip):
                    term(2 + i * strip + g, i * strip + g)

            for x in (0, 1, nx - 2, nx - 1):
                term(x, place(x, True))

        for which, owner in enumerate((ngy // 2 - 1, ngy // 2)):
            @pl.when(iy == owner)
            def _():
                for to in range(ngy):
                    if to != owner:
                        fault_copy(which, to).start()
                frecv[which] = fsend[:, owner * owned:(owner + 1) * owned, :]

        slot = lax.broadcasted_iota(jnp.int32, (1, nz), 1)

        def spread(parts):
            spots = jnp.zeros((1, nz), jnp.float32)
            for j, part, by in parts:
                whole = jnp.sum(jnp.sum(part, axis=0, keepdims=True), axis=1, keepdims=True)
                spots = spots + jnp.where(slot == j, whole * by, 0.0)
            return spots

        unit = 1.0 / 12.0
        early = spread([(0, t0, 1.0), (1, s0, unit), (2, s1, unit), (3, s2, unit), (4, s3, unit)])
        s4 = inside(2, 0, PIECES, zero)
        s4 = borders(2, s4)
        pass_on(len(rounds) - 2)
        s4 = last_planes(s4)
        red[me] = early + spread([(5, s4, unit)])
        hear(known.at[len(rounds) - 1], rounds[-1])

        def sum_copy(who):
            return pltpu.make_async_remote_copy(
                red.at[me], red.at[me], rs_sem, rr_sem, device_id=who, device_id_type=MESH)

        others = [(x, y, z) for y in reversed(ys) for x in reversed(xs) for z in reversed(zs)][:-1]
        for who in others:
            sum_copy(who).start()

        for which, owner in enumerate((ngy // 2 - 1, ngy // 2)):
            @pl.when(iy != owner)
            def _():
                fault_copy(which, owner).wait_recv()
        for k in range(3):
            sent(k)

        @pl.when(ix < ngx - 1)
        def _():
            d_copy().wait_send()
            q_copy().wait_send()
        for which, owner in enumerate((ngy // 2 - 1, ngy // 2)):
            @pl.when(iy == owner)
            def _():
                for to in range(ngy):
                    if to != owner:
                        fault_copy(which, to).wait_send()

        arrived = red.at[pl.ds(0, count - 1)]
        everyone = pltpu.make_async_remote_copy(
            arrived, arrived, rs_sem, rr_sem, device_id=others[0], device_id_type=MESH)
        everyone.wait_recv()
        sums = jnp.sum(red[...], axis=0)
        sums = [jnp.sum(jnp.where(slot == j, sums, 0.0), axis=1, keepdims=True) for j in range(6)]
        coefs = solve(sums[0], sums[1:])
        for j in range(3):
            coef_ref[j:j + 1, :] = jnp.broadcast_to(coefs[j], (1, nz))
        everyone.wait_send()

    return kernel


def blend(u0, u1, u2, coef_ref, fault, pre_ref, state_ref, norm_ref, out, slip, obuf, sbuf, out_sem):
    nx, ny, nz = obuf.shape
    coefs = [coef_ref[j:j + 1, :] for j in range(3)]

    def out_copy(c):
        part = pl.ds(c * CHUNK, CHUNK)
        return pltpu.make_async_copy(obuf.at[part], out.at[part], out_sem.at[c])

    slip_copy = pltpu.make_async_copy(sbuf, slip, out_sem.at[nx // CHUNK])

    def mixed(c):
        @pl.loop(0, CHUNK // 4)
        def _(i):
            for g in range(4):
                x = c * CHUNK + i * 4 + g
                for t in range(PAD, PAD + ny, 8):
                    rows = slice(t, t + 8)
                    obuf[x, t - PAD:t - PAD + 8] = (
                        coefs[0] * u0[x + 2, rows, :] + coefs[1] * u1[x + 2, rows, :]
                        + coefs[2] * u2[x + 2, rows, :])
        out_copy(c).start()

    mixed(0)
    traction = sum(coefs[j] * (fault[0, j] + fault[1, j]) for j in range(3))
    arg = (pre_ref[...] + 2.0 * traction) / norm_ref[...]
    half = jnp.float32(-0.6931471805599453)
    small = arg * (1.0 + arg * arg * (1.0 / 6.0) * (1.0 + arg * arg * 0.05))
    sinh = jnp.where(jnp.abs(arg) < 0.25, small, jnp.exp(arg + half) - jnp.exp(half - arg))
    sbuf[...] = jnp.exp(-state_ref[...]) * sinh
    slip_copy.start()
    pl.loop(1, nx // CHUNK)(mixed)
    slip_copy.wait()
    for c in range(nx // CHUNK):
        out_copy(c).wait()


def solution(mesh):
    sizes = tuple(mesh.shape[a] for a in AXES)
    assert sizes[1] % 2 == 0 and sizes[2] == 2

    def per_device(load, stiffness, prestress, state_var, normal_a):
        nx, ny, nz = load.shape
        assert nx % CHUNK == 0 and nx % 4 == 0 and 2 * nx <= nz and (nx - 4) % PIECES == 0 and ny % 8 == 0 and ny >= 32
        f32 = jnp.float32
        count = sizes[0] * sizes[1] * sizes[2]
        padded = (nx + 4, ny + 2 * PAD, nz)
        vmem = pl.BlockSpec(memory_space=pltpu.VMEM)
        hbm = pl.BlockSpec(memory_space=pltpu.HBM)
        dma = pltpu.SemaphoreType.DMA
        u0, u1, u2, coefs, fault = pl.pallas_call(
            make_kernel(sizes),
            out_shape=(
                pltpu.VMEM(padded, f32),
                pltpu.VMEM(padded, f32),
                pltpu.VMEM(padded, f32),
                pltpu.VMEM((8, nz), f32),
                pltpu.VMEM((2, 3, nx // sizes[1], nz), f32),
            ),
            in_specs=[hbm, hbm],
            out_specs=(vmem,) * 5,
            scratch_shapes=[
                pltpu.VMEM((nx, ny, nz), f32),
                pltpu.VMEM((nx, ny, nz), f32),
                pltpu.VMEM((3, 2, nx, 2, nz), f32),
                pltpu.VMEM((3, 2, nx, 2, nz), f32),
                pltpu.VMEM((3, PIECES, ny - 16, nz), f32),
                pltpu.VMEM((3, PIECES, ny - 16, nz), f32),
                pltpu.VMEM((3, ny + 16, nz), f32),
                pltpu.VMEM((3, ny + 16, nz), f32),
                pltpu.VMEM((2, 2 * nz, 2 * nz), jnp.bfloat16),
                pltpu.VMEM((nx, ny, nz), f32),
                pltpu.VMEM((3, nx, nz), f32),
                pltpu.VMEM((count, 1, nz), f32),
                pltpu.VMEM((2, ny, nz), f32),
                pltpu.VMEM((2, ny, nz), f32),
                pltpu.VMEM((2, ny, nz), f32),
                dma((2 + PIECES,)),
                dma,
                dma((2, 2)),
                dma((2, 3, 2)),
                dma((2, PIECES + 1)),
                dma((2,)),
                dma,
                dma,
                dma((2,)),
                pltpu.SemaphoreType.REGULAR((len(line_rounds(sizes)) + 2,)),
            ],
            compiler_params=pltpu.CompilerParams(
                collective_id=0, has_side_effects=True, vmem_limit_bytes=54 * 2**20),
        )(load, stiffness)
        displacement, slip = pl.pallas_call(
            blend,
            out_shape=(
                jax.ShapeDtypeStruct(load.shape, f32),
                jax.ShapeDtypeStruct(prestress.shape, f32),
            ),
            in_specs=[vmem] * 8,
            out_specs=(hbm, hbm),
            scratch_shapes=[
                pltpu.VMEM((nx, ny, nz), f32),
                pltpu.VMEM(prestress.shape, f32),
                dma((nx // CHUNK + 1,)),
            ],
            compiler_params=pltpu.CompilerParams(vmem_limit_bytes=8 * 2**20),
        )(u0, u1, u2, coefs, fault, prestress, state_var, normal_a)
        return displacement, slip

    placed = (
        P("gx", "gy", "gz"),
        P("gx", "gy", "gz"),
        P(("gx", "gy"), "gz"),
        P(("gx", "gy"), "gz"),
        P(("gx", "gy"), "gz"),
    )
    return jax.shard_map(
        per_device,
        mesh=mesh,
        in_specs=placed,
        out_specs=(P("gx", "gy", "gz"), P(("gx", "gy"), "gz")),
        check_vma=False,
    )
```

```python
import jax
import jax.numpy as jnp
from jax import lax
from jax.experimental import pallas as pl
from jax.experimental.pallas import tpu as pltpu
from jax.sharding import PartitionSpec as P

MESH = pl.DeviceIdType.MESH
AXES = ("gx", "gy", "gz")
PAD = 8
CHUNK = 8
PIECES = 4


def total(values):
    return jnp.sum(values.reshape(-1, 8, values.shape[-1]), axis=0)


def solve(t0, s):
    t1 = t0 - s[0]
    t2 = t1 - s[1]
    tiny = 1e-7
    p0 = s[0]
    l10 = s[1] / p0
    l20 = s[2] / p0
    p1 = s[2] - l10 * s[1]
    q = s[3] - l20 * s[1]
    ok1 = p1 > tiny * s[2]
    i1 = jnp.where(ok1, 1.0 / jnp.where(ok1, p1, 1.0), 0.0)
    l21 = q * i1
    p2 = s[4] - l20 * s[2] - l21 * q
    ok2 = ok1 & (p2 > tiny * s[4])
    i2 = jnp.where(ok2, 1.0 / jnp.where(ok2, p2, 1.0), 0.0)
    y1 = t1 - l10 * t0
    y2 = t2 - l20 * t0 - l21 * y1
    c2 = y2 * i2
    c1 = y1 * i1 - l21 * c2
    c0 = t0 / p0 - l10 * c1 - l20 * c2
    return c0, c1, c2


def divisor(n, most):
    return max(m for m in range(1, most + 1) if n % m == 0)


def halves(values):
    high = values.astype(jnp.bfloat16)
    return high, (values - high.astype(jnp.float32)).astype(jnp.bfloat16)


def line_rounds(sizes):
    hops = [1]
    while 2 * hops[-1] < max(sizes[:2]) - 1:
        hops.append(2 * hops[-1])
    return hops


def make_kernel(sizes):
    ngx, ngy, ngz = sizes
    count = ngx * ngy * ngz

    def kernel(load, stiff, u0, u1, u2, coef_ref, frecv,
               b, d, ysend, yrecv, zsend, zrecv, rsend, rrecv, band, zterm, fsend, red,
               dhalo, qsend, qhalo,
               in_sem, send_sem, x_sem, y_sem, z_sem, fr_sem, rs_sem, rr_sem, q_sem,
               known):
        nx, ny, nz = b.shape
        us = (u0, u1, u2)
        ix, iy, iz = (lax.axis_index(a) for a in AXES)
        me = (ix * ngy + iy) * ngz + iz
        half = (nx - 4) // 2
        piece = (nx - 4) // PIECES
        window = divisor(piece, 5)
        run_y = divisor(half, 30)
        strip = divisor(half, 6)
        mid = tuple(range(8, ny - 8, 8))
        ends = (0, ny - 8)
        full = tuple(range(0, ny, 8))

        def around(spot, size):
            moved = [spot + n for n in range(size)]
            return [spot] + [jnp.where(m >= size, m - size, m) for m in moved[1:]]

        xs, ys, zs = around(ix, ngx), around(iy, ngy), around(iz, ngz)

        sources = ((load, b), (stiff, d))
        for src, dst in sources:
            for at in (0, nx - 2):
                pltpu.make_async_copy(src.at[at:at + 2], dst.at[at:at + 2], in_sem.at[0]).start()
        for src, dst in sources:
            for at in ends:
                pltpu.make_async_copy(
                    src.at[2:nx - 2, at:at + 8], dst.at[2:nx - 2, at:at + 8], in_sem.at[1]).start()
        for n in range(PIECES):
            part = pl.ds(2 + n * piece, piece)
            for src, dst in sources:
                pltpu.make_async_copy(
                    src.at[part, 8:ny - 8], dst.at[part, 8:ny - 8], in_sem.at[2 + n]).start()

        def loaded(ref, n):
            pltpu.make_async_copy(ref, ref, in_sem.at[n]).wait()

        barrier = pltpu.get_barrier_semaphore()
        def lines(radius, axes=(0, 1)):
            spots = (ix, iy, iz)
            for axis in axes:
                for gap in range(1, min(radius, sizes[axis] - 1) + 1):
                    for step in (-gap, gap):
                        to = spots[axis] + step
                        yield (to >= 0 if step < 0 else to < sizes[axis],
                               tuple(to if n == axis else spot for n, spot in enumerate(spots)))

        def tell(sem, who):
            for there, device in who:
                @pl.when(there)
                def _():
                    pl.semaphore_signal(sem, inc=1, device_id=device, device_id_type=MESH)

        def hear(sem, who):
            pl.semaphore_wait(sem, sum(jnp.where(there, 1, 0) for there, _ in who))

        rounds = ([tuple(lines(hop)) for hop in line_rounds(sizes)]
                  + [tuple(lines(ngy, (1,))), tuple(lines(ngz, (2,)))])
        near = tuple(lines(1, (0, 1, 2)))
        tell(barrier, near)

        zero_plane = jnp.zeros((2, ny, nz), jnp.float32)
        zero_rows = jnp.zeros((nx, 2, nz), jnp.float32)
        for k in range(3):
            @pl.when(ix == 0)
            def _():
                us[k][0:2, PAD:PAD + ny, :] = zero_plane
            @pl.when(ix == ngx - 1)
            def _():
                us[k][nx + 2:nx + 4, PAD:PAD + ny, :] = zero_plane
            @pl.when(iy == 0)
            def _():
                yrecv[k, 0] = zero_rows
            @pl.when(iy == ngy - 1)
            def _():
                yrecv[k, 1] = zero_rows

        row = lax.broadcasted_iota(jnp.int32, (nz, nz), 0)
        col = lax.broadcasted_iota(jnp.int32, (nz, nz), 1)
        far = jnp.bitwise_and(col, 1) + jnp.where(iz == 0, nz, -2)

        def weights(gap, near):
            return jnp.where(near(gap) == 1, 16.0, 0.0) - jnp.where(near(gap) == 2, 1.0, 0.0)

        own = weights(col - row, jnp.abs)
        up = weights(col - row, lambda g: g)
        out = weights(far - row, jnp.abs).astype(jnp.bfloat16)
        for which, part in enumerate((own, up)):
            for n in range(2):
                band[which, n * nz:(n + 1) * nz, 0:nz] = part.astype(jnp.bfloat16)
                band[which, n * nz:(n + 1) * nz, nz:2 * nz] = out

        lane = lax.broadcasted_iota(jnp.int32, (8, nz), 1)
        pair = lane // 2
        edge_low = jnp.where(iz == 0, nz - 2, 0)
        at_edge = (lane >= edge_low) & (lane < edge_low + 2)
        at_upper = at_edge & (iz == 1)

        def xcopy(k, side):
            u = us[k]
            rows = pl.ds(PAD, ny)
            if side == 0:
                src, dst, to = u.at[2:4, rows], u.at[nx + 2:nx + 4, rows], ix - 1
            else:
                src, dst, to = u.at[nx:nx + 2, rows], u.at[0:2, rows], ix + 1
            return pltpu.make_async_remote_copy(
                src, dst, send_sem, x_sem.at[k, side],
                device_id=(to, iy, iz), device_id_type=MESH)

        def ycopy(k, n, side):
            to = iy - 1 if side == 0 else iy + 1
            part = pl.ds(n * half, half) if n < 2 else pl.ds(nx - 4, 4)
            return pltpu.make_async_remote_copy(
                ysend.at[k, side, part], yrecv.at[k, 1 - side, part], send_sem,
                y_sem.at[k % 2, n, side], device_id=(ix, to, iz), device_id_type=MESH)

        def place(x, rim):
            if not rim:
                return x - 2
            return x if x >= nx - 2 else nx - 4 + x

        def zcopy(k, n):
            rim = isinstance(n, int) and n == PIECES
            src, dst = (rsend.at[k], rrecv.at[k]) if rim else (zsend.at[k, n], zrecv.at[k, n])
            return pltpu.make_async_remote_copy(
                src, dst, send_sem, z_sem.at[k % 2, n],
                device_id=(ix, iy, 1 - iz), device_id_type=MESH)

        def sending(spot, size, side):
            return spot > 0 if side == 0 else spot < size - 1

        def receiving(spot, size, side):
            return spot < size - 1 if side == 0 else spot > 0

        def sides(k):
            return (0,) if k == 2 else (0, 1)

        def d_copy():
            return pltpu.make_async_remote_copy(
                d.at[0:2], dhalo, send_sem, q_sem.at[0],
                device_id=(ix - 1, iy, iz), device_id_type=MESH)

        def q_copy():
            return pltpu.make_async_remote_copy(
                qsend, qhalo, send_sem, q_sem.at[1],
                device_id=(ix - 1, iy, iz), device_id_type=MESH)

        def each(make, k, n, spot, size, test, act):
            for side in sides(k):
                @pl.when(test(spot, size, side))
                def _():
                    act(make(k, n, side))

        def start_x(k):
            odd = lax.rem(ix, 2) == 1
            for side, turn in ((1, odd), (0, None), (1, jnp.logical_not(odd))):
                go = sending(ix, ngx, side)
                @pl.when(go if turn is None else go & turn)
                def _():
                    xcopy(k, side).start()

        def start_y(k, n):
            each(ycopy, k, n, iy, ngy, sending, lambda c: c.start())

        def wait_y(k, n):
            each(ycopy, k, n, iy, ngy, receiving, lambda c: c.wait_recv())

        def wait_x(k, n=0):
            each(lambda k, n, side: xcopy(k, side), k, n, ix, ngx, receiving, lambda c: c.wait_recv())

        def sent(k):
            for n in range(3):
                if n == 0 and k < 2:
                    each(lambda k, n, side: xcopy(k, side), k, n, ix, ngx, sending, lambda c: c.wait_send())
                each(ycopy, k, n, iy, ngy, sending, lambda c: c.wait_send())
            for n in range(PIECES + 1):
                zcopy(k, n).wait_send()

        def along_z(k, values, rows):
            high, low = halves(values)
            lhs = jnp.concatenate([high, low], axis=1)
            found = jnp.dot(lhs, band[1 if k == 2 else 0], preferred_element_type=jnp.float32)
            return found[:, :nz].reshape(-1, rows, nz), found[:, nz:].reshape(-1, rows, nz)

        def picked(k, x, n, lo, hi, packed):
            rows = hi - lo
            values = us[k][pl.ds(x + 2, n), PAD + lo:PAD + hi, :].reshape(n * rows, nz)
            own, out = along_z(k, values, rows)
            zterm[pl.ds(x, n), lo:hi, :] = own
            for g in range(n):
                keep = jnp.concatenate([pair] * (rows // 8), axis=0) == x + g
                packed = jnp.where(keep, out[g], packed)
            return packed

        def rims_z(k):
            low = high = jnp.zeros((8, nz), jnp.float32)
            for h in range(2):
                low = picked(k, 2 + h * half, half, 0, 8, low)
                high = picked(k, 2 + h * half, half, ny - 8, ny, high)
            rsend[k, 0:8] = low
            rsend[k, 8:16] = high
            packed = jnp.zeros((ny, nz), jnp.float32)
            for at in (0, nx - 2):
                packed = picked(k, at, 2, 0, ny, packed)
            rsend[k, 16:16 + ny] = packed
            zcopy(k, PIECES).start()

        def put(k, x, slot, t, value):
            us[k][x + 2, PAD + t:PAD + t + 8, :] = value
            if t == 0:
                ysend[k, 0, slot] = value[0:2]
            if t == ny - 8:
                ysend[k, 1, slot] = value[6:8]

        def scale(x, n, tiles, t0, slot=None):
            for g in range(n):
                for t in tiles:
                    rows = slice(t, t + 8)
                    inv = 1.0 / (7.5 + d[x + g, rows])
                    rhs = b[x + g, rows]
                    value = inv * rhs
                    d[x + g, rows] = inv * (1.0 / 12.0)
                    b[x + g, rows] = 12.0 * rhs
                    put(0, x + g, x + g - 2 if slot is None else slot, t, value)
                    t0 = t0 + value * rhs
            return t0

        def shift_of(x):
            return jnp.bitwise_and(jnp.where(iz == 0, nz - 2, nz) - 2 * x, nz - 1)

        def stencil(k, x, n, tiles, source, carry, rim=False):
            u = us[k]
            for t in tiles:
                lo, hi = PAD + t, PAD + t + 8
                packed = source(t)
                line = [u[x + j, lo:hi, :] if k < 2 or j > 1 else None for j in range(n + 4)]
                for g in range(n):
                    at = x + g
                    rows = slice(t, t + 8)
                    c = line[g + 2]
                    z = zterm[at, rows] + jnp.where(
                        at_edge if k < 2 else at_upper, pltpu.roll(packed, shift_of(at), 1), 0.0)
                    if k < 2:
                        even, odd = carry
                        one = ((line[g + 1] + line[g + 3])
                               + (u[at + 2, lo - 1:hi - 1, :] + u[at + 2, lo + 1:hi + 1, :]))
                        two = ((line[g] + line[g + 4])
                               + (u[at + 2, lo - 2:hi - 2, :] + u[at + 2, lo + 2:hi + 2, :]))
                        w = (16.0 * one - two) + z
                        fresh = d[at, rows] * w
                        even = even + c * (b[at, rows] - w)
                        odd = odd + (c - fresh) * w
                        b[at, rows] = w
                        put(k + 1, at, place(at, rim), t, fresh)
                        carry = even, odd
                    else:
                        one = line[g + 3] + u[at + 2, lo + 1:hi + 1, :]
                        two = line[g + 4] + u[at + 2, lo + 2:hi + 2, :]
                        w = (16.0 * one - two) + z
                        carry = carry + c * (b[at, rows] - (w + w))
            return carry

        def pack(k, n):
            packed = picked(k, 2 + n * piece, piece, 8, ny - 8, jnp.zeros((ny - 16, nz), jnp.float32))
            zsend[k, n] = packed
            zcopy(k, n).start()

        def inside(k, first, last, carry):
            def part(n, carry):
                zcopy(k, n).wait_recv()
                x = 2 + n * piece
                for g in range(0, piece, window):
                    carry = stencil(k, x + g, window, mid, lambda t: zrecv[k, n, t - 8:t], carry)
                if k < 2:
                    pack(k + 1, n)
                return carry

            return lax.fori_loop(first, last, part, carry)

        zero = jnp.zeros((8, nz), jnp.float32)

        loaded(b.at[0:8], 0)
        t0 = lax.fori_loop(0, 4, lambda n, c: scale(
            jnp.where(n < 2, n, nx - 4 + n), 1, full, c, nx - 4 + n), zero)
        loaded(b.at[2:nx - 2, 0:32], 1)
        for h in range(2):
            t0 = lax.fori_loop(
                0, half // strip, lambda n, c: scale(2 + h * half + n * strip, strip, ends, c), t0)
            if h == 0:
                hear(barrier, near)
                start_x(0)
            start_y(0, h)
        start_y(0, 2)
        tell(known.at[0], rounds[0])
        rims_z(0)

        def fresh_part(n, t0):
            loaded(b.at[0:2 * piece, 8:ny - 8], 2 + n)
            t0 = scale(2 + n * piece, piece, mid, t0)
            pack(0, n)
            return t0

        t0 = lax.fori_loop(0, PIECES, fresh_part, t0)

        def row_in(k, x, slot, side_set):
            if 0 in side_set and k < 2:
                us[k][x + 2, PAD - 2:PAD, :] = yrecv[k, 0, slot]
            if 1 in side_set:
                us[k][x + 2, PAD + ny:PAD + ny + 2, :] = yrecv[k, 1, slot]

        def border(k, h, carry):
            wait_y(k, h)

            @pl.loop(0, half // strip)
            def _(i):
                for g in range(strip):
                    slot = h * half + i * strip + g
                    row_in(k, slot + 2, slot, (0, 1))

            def piece_of(i, carry):
                return stencil(k, 2 + h * half + i * run_y, run_y, ends,
                               lambda t: rrecv[k, 0:8] if t == 0 else rrecv[k, 8:16], carry)

            carry = lax.fori_loop(0, half // run_y, piece_of, carry)
            if k < 2:
                start_y(k + 1, h)
            return carry

        def outer(k, n, carry):
            for x in (0, 1, nx - 2, nx - 1):
                row_in(k, x, place(x, True), (n,))
            for at in (0, nx - 2):
                carry = stencil(k, at, 2, full[n * len(full) // 2:(n + 1) * len(full) // 2],
                                lambda t: rrecv[k, 16 + t:24 + t], carry, True)
            return carry

        def lacking():
            for x in (0, 1, nx - 2, nx - 1):
                row_in(1, x, place(x, True), (0, 1))

            @pl.when(ix > 0)
            def _():
                for t in full:
                    lo, hi = PAD + t, PAD + t + 8
                    line = [u1[j + 2, lo:hi, :] for j in range(4)]
                    for g in range(2):
                        z = zterm[g, t:t + 8] + jnp.where(
                            at_edge, pltpu.roll(rrecv[1, 16 + t:24 + t], shift_of(g), 1), 0.0)
                        one = line[g + 1] + (u1[g + 2, lo - 1:hi - 1, :] + u1[g + 2, lo + 1:hi + 1, :])
                        two = line[g + 2] + (u1[g + 2, lo - 2:hi - 2, :] + u1[g + 2, lo + 2:hi + 2, :])
                        if g == 1:
                            one = one + line[0]
                        qsend[g, t:t + 8] = (16.0 * one - two) + z
                q_copy().start()

        def last_planes(carry):
            for x in (0, 1, nx - 2, nx - 1):
                row_in(2, x, place(x, True), (1,))
            carry = stencil(2, 0, 2, full, lambda t: rrecv[2, 16 + t:24 + t], carry, True)

            @pl.when(ix < ngx - 1)
            def _():
                d_copy().wait_recv()
                q_copy().wait_recv()
                for t in full:
                    rows, lines = slice(t, t + 8), slice(PAD + t, PAD + t + 8)
                    first, second = u1[nx + 1, lines, :], u1[nx, lines, :]
                    u2[nx + 2, lines, :] = dhalo[0, rows] * (qhalo[0, rows] + (16.0 * first - second))
                    u2[nx + 3, lines, :] = dhalo[1, rows] * (qhalo[1, rows] - first)

            return stencil(2, nx - 2, 2, full, lambda t: rrecv[2, 16 + t:24 + t], carry, True)

        def borders(k, carry):
            zcopy(k, PIECES).wait_recv()
            for h in range(2):
                carry = border(k, h, carry)
            wait_y(k, 2)
            return carry

        def pass_on(n):
            hear(known.at[n], rounds[n])
            if n + 1 < len(rounds):
                tell(known.at[n + 1], rounds[n + 1])

        @pl.when(ix > 0)
        def _():
            d_copy().start()

        lead = PIECES - 1
        state = inside(0, 0, lead, (zero, zero))
        for n in range(len(rounds) - 3):
            pass_on(n)
        state = borders(0, state)
        wait_x(0)
        state = outer(0, 1, outer(0, 0, state))
        start_x(1)
        start_y(1, 2)
        s0, s1 = inside(0, lead, PIECES, state)
        rims_z(1)
        state = inside(1, 0, lead, (zero, zero))
        pass_on(len(rounds) - 3)
        state = borders(1, state)
        lacking()
        state = inside(1, lead, PIECES, state)
        wait_x(1)
        state = outer(1, 0, state)
        start_y(2, 2)
        s2, s3 = outer(1, 1, state)
        rims_z(2)

        owned = nx // ngy
        below = iy == ngy // 2 - 1
        above = iy == ngy // 2

        def fault_copy(which, to):
            return pltpu.make_async_remote_copy(
                fsend.at[:, pl.ds(to * owned, owned), :], frecv.at[which], send_sem, fr_sem.at[which],
                device_id=(ix, to, iz), device_id_type=MESH)

        @pl.when(below | above)
        def _():
            edge = jnp.where(below, 1, 0)
            front = jnp.where(below, 1.0 / 24.0, 27.0 / 24.0)
            close = jnp.where(below, -27.0 / 24.0, -1.0 / 24.0)

            def term(x, slot):
                for j in range(3):
                    rows = ysend[j, edge, slot]
                    fsend[j, pl.ds(x, 1), :] = front * rows[0:1] + close * rows[1:2]

            @pl.loop(0, (nx - 4) // strip)
            def _(i):
                for g in range(strip):
                    term(2 + i * strip + g, i * strip + g)

            for x in (0, 1, nx - 2, nx - 1):
                term(x, place(x, True))

        for which, owner in enumerate((ngy // 2 - 1, ngy // 2)):
            @pl.when(iy == owner)
            def _():
                for to in range(ngy):
                    if to != owner:
                        fault_copy(which, to).start()
                frecv[which] = fsend[:, owner * owned:(owner + 1) * owned, :]

        slot = lax.broadcasted_iota(jnp.int32, (1, nz), 1)

        def spread(parts):
            spots = jnp.zeros((1, nz), jnp.float32)
            for j, part, by in parts:
                whole = jnp.sum(jnp.sum(part, axis=0, keepdims=True), axis=1, keepdims=True)
                spots = spots + jnp.where(slot == j, whole * by, 0.0)
            return spots

        unit = 1.0 / 12.0
        early = spread([(0, t0, 1.0), (1, s0, unit), (2, s1, unit), (3, s2, unit), (4, s3, unit)])
        s4 = inside(2, 0, PIECES, zero)
        pass_on(len(rounds) - 2)
        s4 = borders(2, s4)
        s4 = last_planes(s4)
        red[me] = early + spread([(5, s4, unit)])
        hear(known.at[len(rounds) - 1], rounds[-1])

        def sum_copy(who):
            return pltpu.make_async_remote_copy(
                red.at[me], red.at[me], rs_sem, rr_sem, device_id=who, device_id_type=MESH)

        others = [(x, y, z) for y in reversed(ys) for x in reversed(xs) for z in reversed(zs)][:-1]
        for who in others:
            sum_copy(who).start()

        for which, owner in enumerate((ngy // 2 - 1, ngy // 2)):
            @pl.when(iy != owner)
            def _():
                fault_copy(which, owner).wait_recv()
        for k in range(3):
            sent(k)

        @pl.when(ix > 0)
        def _():
            d_copy().wait_send()
            q_copy().wait_send()
        for which, owner in enumerate((ngy // 2 - 1, ngy // 2)):
            @pl.when(iy == owner)
            def _():
                for to in range(ngy):
                    if to != owner:
                        fault_copy(which, to).wait_send()

        arrived = red.at[pl.ds(0, count - 1)]
        everyone = pltpu.make_async_remote_copy(
            arrived, arrived, rs_sem, rr_sem, device_id=others[0], device_id_type=MESH)
        everyone.wait_recv()
        sums = jnp.sum(red[...], axis=0)
        sums = [jnp.sum(jnp.where(slot == j, sums, 0.0), axis=1, keepdims=True) for j in range(6)]
        coefs = solve(sums[0], sums[1:])
        for j in range(3):
            coef_ref[j:j + 1, :] = jnp.broadcast_to(coefs[j], (1, nz))
        everyone.wait_send()

    return kernel


def blend(u0, u1, u2, coef_ref, fault, pre_ref, state_ref, norm_ref, out, slip, obuf, sbuf, out_sem):
    nx, ny, nz = obuf.shape
    coefs = [coef_ref[j:j + 1, :] for j in range(3)]

    def out_copy(c):
        part = pl.ds(c * CHUNK, CHUNK)
        return pltpu.make_async_copy(obuf.at[part], out.at[part], out_sem.at[c])

    slip_copy = pltpu.make_async_copy(sbuf, slip, out_sem.at[nx // CHUNK])

    def mixed(c):
        @pl.loop(0, CHUNK // 4)
        def _(i):
            for g in range(4):
                x = c * CHUNK + i * 4 + g
                for t in range(PAD, PAD + ny, 8):
                    rows = slice(t, t + 8)
                    obuf[x, t - PAD:t - PAD + 8] = (
                        coefs[0] * u0[x + 2, rows, :] + coefs[1] * u1[x + 2, rows, :]
                        + coefs[2] * u2[x + 2, rows, :])
        out_copy(c).start()

    mixed(0)
    traction = sum(coefs[j] * (fault[0, j] + fault[1, j]) for j in range(3))
    arg = (pre_ref[...] + 2.0 * traction) / norm_ref[...]
    half = jnp.float32(-0.6931471805599453)
    small = arg * (1.0 + arg * arg * (1.0 / 6.0) * (1.0 + arg * arg * 0.05))
    sinh = jnp.where(jnp.abs(arg) < 0.25, small, jnp.exp(arg + half) - jnp.exp(half - arg))
    sbuf[...] = jnp.exp(-state_ref[...]) * sinh
    slip_copy.start()
    pl.loop(1, nx // CHUNK)(mixed)
    slip_copy.wait()
    for c in range(nx // CHUNK):
        out_copy(c).wait()


def solution(mesh):
    sizes = tuple(mesh.shape[a] for a in AXES)
    assert sizes[1] % 2 == 0 and sizes[2] == 2

    def per_device(load, stiffness, prestress, state_var, normal_a):
        nx, ny, nz = load.shape
        assert nx % CHUNK == 0 and nx % 4 == 0 and 2 * nx <= nz and (nx - 4) % PIECES == 0 and ny % 8 == 0 and ny >= 32
        f32 = jnp.float32
        count = sizes[0] * sizes[1] * sizes[2]
        padded = (nx + 4, ny + 2 * PAD, nz)
        vmem = pl.BlockSpec(memory_space=pltpu.VMEM)
        hbm = pl.BlockSpec(memory_space=pltpu.HBM)
        dma = pltpu.SemaphoreType.DMA
        u0, u1, u2, coefs, fault = pl.pallas_call(
            make_kernel(sizes),
            out_shape=(
                pltpu.VMEM(padded, f32),
                pltpu.VMEM(padded, f32),
                pltpu.VMEM(padded, f32),
                pltpu.VMEM((8, nz), f32),
                pltpu.VMEM((2, 3, nx // sizes[1], nz), f32),
            ),
            in_specs=[hbm, hbm],
            out_specs=(vmem,) * 5,
            scratch_shapes=[
                pltpu.VMEM((nx, ny, nz), f32),
                pltpu.VMEM((nx, ny, nz), f32),
                pltpu.VMEM((3, 2, nx, 2, nz), f32),
                pltpu.VMEM((3, 2, nx, 2, nz), f32),
                pltpu.VMEM((3, PIECES, ny - 16, nz), f32),
                pltpu.VMEM((3, PIECES, ny - 16, nz), f32),
                pltpu.VMEM((3, ny + 16, nz), f32),
                pltpu.VMEM((3, ny + 16, nz), f32),
                pltpu.VMEM((2, 2 * nz, 2 * nz), jnp.bfloat16),
                pltpu.VMEM((nx, ny, nz), f32),
                pltpu.VMEM((3, nx, nz), f32),
                pltpu.VMEM((count, 1, nz), f32),
                pltpu.VMEM((2, ny, nz), f32),
                pltpu.VMEM((2, ny, nz), f32),
                pltpu.VMEM((2, ny, nz), f32),
                dma((2 + PIECES,)),
                dma,
                dma((2, 2)),
                dma((2, 3, 2)),
                dma((2, PIECES + 1)),
                dma((2,)),
                dma,
                dma,
                dma((2,)),
                pltpu.SemaphoreType.REGULAR((len(line_rounds(sizes)) + 2,)),
            ],
            compiler_params=pltpu.CompilerParams(
                collective_id=0, has_side_effects=True, vmem_limit_bytes=54 * 2**20),
        )(load, stiffness)
        displacement, slip = pl.pallas_call(
            blend,
            out_shape=(
                jax.ShapeDtypeStruct(load.shape, f32),
                jax.ShapeDtypeStruct(prestress.shape, f32),
            ),
            in_specs=[vmem] * 8,
            out_specs=(hbm, hbm),
            scratch_shapes=[
                pltpu.VMEM((nx, ny, nz), f32),
                pltpu.VMEM(prestress.shape, f32),
                dma((nx // CHUNK + 1,)),
            ],
            compiler_params=pltpu.CompilerParams(vmem_limit_bytes=8 * 2**20),
        )(u0, u1, u2, coefs, fault, prestress, state_var, normal_a)
        return displacement, slip

    placed = (
        P("gx", "gy", "gz"),
        P("gx", "gy", "gz"),
        P(("gx", "gy"), "gz"),
        P(("gx", "gy"), "gz"),
        P(("gx", "gy"), "gz"),
    )
    return jax.shard_map(
        per_device,
        mesh=mesh,
        in_specs=placed,
        out_specs=(P("gx", "gy", "gz"), P(("gx", "gy"), "gz")),
        check_vma=False,
    )
```
